256 devices in a mesh: dp: 8 (over x, y_lo), tp: 32 (over y_hi, z, core).
Axes of the slice: x: 4, y: 4 (y_hi: 2, y_lo: 2; y = y_hi * 2 + y_lo), z: 8, core: 2. Of those that a mesh axis runs over, the one named last changes fastest.
Arguments:
- proj_in: bfloat16 [1, 32768, 8192], P(None, 'dp', 'tp'), may hold values from -6 to 6
- kv_grad: bfloat16 [1, 32768, 2048], P(None, ('dp', 'tp')), may hold values from -0.75 to 0.75
- normed: bfloat16 [1, 32768, 8192], P(None, ('dp', 'tp')), may hold values from -6 to 6
- norm_grad: bfloat16 [1, 32768, 8192], P(None, ('dp', 'tp')), may hold values from -0.6 to 0.6
- first_moment: float32 [1, 8192, 2048], P(None, 'tp', 'dp'), may hold values from -0.6 to 0.6
- second_moment: float32 [1, 8192, 2048], P(None, 'tp', 'dp'), may hold values from 0.002 to 0.02
Outputs:
- new_first: float32 [1, 8192, 2048], P(None, 'tp', 'dp')
- new_second: float32 [1, 8192, 2048], P(None, 'tp', 'dp')
- adam_step: float32 [1, 8192, 2048], P(None, 'tp', 'dp')
- gain_grad: float32 [1, 8192], replicated
The draws below stay inside these ranges and needn't reach their ends.
All inputs are finite; a program needn't handle non-finite values.
Results may differ from the reference program's by a relative error of at most 0.0003.
Values may be sent and summed in bfloat16 or wider, within the bound.
No kernel may reach another device: no remote copies, remote signals or barrier semaphores. Data moves between devices by JAX's collectives and lax.ppermute only.
A program may use at most 128 MiB of HBM per device.

```python
import math
import jax
import jax.numpy as jnp
from jax import lax

D = 8192
KV = 2048
LAYERS = 1
TOK_REP = 4096
TOKENS = 32768
N_DP = 8


def draw_norm_grad(key, part):
    first_key, second_key, third_key = jax.random.split(key, 3)
    values = 0.1 * jax.random.normal(first_key, (LAYERS, TOKENS, D), jnp.float32)
    return jnp.clip(values, -0.6, 0.6).astype(jnp.bfloat16)


def strengthened(result, own_key, source, target, parts, factor):
    def block_of(position):
        return (jnp.arange(result.shape[position]) // (result.shape[position] // parts)).reshape((-1,) + (1,) * (result.ndim - 1 - position))

    one_side = jax.random.permutation(own_key, parts)[block_of(target)]
    second = (block_of(target) + parts // 2) % parts
    return jnp.where((block_of(source) == one_side) | (block_of(source) == second), factor * result, result)


def block_levels(stream_key, dims, shards, least, top_value):
    factor_of, own = 1.0, jax.random.fold_in(stream_key, 6)
    for axis_at, parts in shards:
        draws = jnp.exp(jax.random.uniform(jax.random.fold_in(own, axis_at), (parts,), jnp.float32, least / len(shards), top_value / len(shards)))
        factor_of = factor_of * jnp.repeat(draws, dims[axis_at] // parts).reshape([-1 if axis == axis_at else 1 for axis in range(len(dims))])
    return factor_of


def bell_draw(rng, extent, scale, bound, pieces=(), held_as=jnp.bfloat16):
    loudness = block_levels(rng, extent, pieces, -0.22, 0.18) if pieces else 1.0
    array = jax.random.normal(rng, extent, jnp.float32) * scale * loudness
    return jnp.minimum(jnp.maximum(array, -bound), bound).astype(held_as)


def heavy_noise(key, shape, deviation, limit, cuts, heavy, held_as=jnp.bfloat16):
    drawn = deviation * jax.random.normal(key, shape, jnp.float32)
    if cuts:
        drawn = drawn * block_levels(key, shape, cuts, -0.22, 0.18)
    return jnp.clip(strengthened(drawn, jax.random.fold_in(key, 3), *heavy), -limit, limit).astype(held_as)


def setup_inputs(seed: int = 0) -> dict:
    splits = jax.random.split(jax.random.key(seed), 7)
    return {
        "proj_in": bell_draw(splits[0], (LAYERS, TOKENS, D), 1.0, 6.0, ((1, 8), (2, 32))),
        "kv_grad": heavy_noise(splits[1], (LAYERS, TOKENS, KV), 0.03, 0.75, ((1, 256),), (1, 2, 256, 6.0)),
        "normed": bell_draw(splits[2], (LAYERS, TOKENS, D), 1.0, 6.0, ((1, 256),)),
        "norm_grad": draw_norm_grad(jax.random.fold_in(splits[6], 71), 0),
        "first_moment": bell_draw(splits[4], (LAYERS, D, KV), 0.1, 0.6, ((1, 32), (2, 8)), jnp.float32),
        "second_moment": jnp.clip(jnp.exp(math.log(0.02) - 2.30258502 * jax.random.uniform(splits[5], (LAYERS, D, KV), jnp.float32) ** block_levels(splits[5], (LAYERS, D, KV), ((1, 32), (2, 8)), -0.2, 0.2)), 0.002, 0.02),
    }


beta_one = 0.9
beta_two = 0.95
correct_one = 0.19
correct_two = 0.0975
epsilon = 1e-08

def reference(proj_in, kv_grad, normed, norm_grad, first_moment, second_moment):
    firsts = []
    seconds = []
    updates = []
    for layer_id in range(LAYERS):
        running = jnp.zeros((D, KV), jnp.float32)
        for replica in range(N_DP):
            inputs = proj_in[layer_id, replica * TOK_REP:(replica + 1) * TOK_REP]
            grad_rows = kv_grad[layer_id, replica * TOK_REP:(replica + 1) * TOK_REP]
            product = lax.dot_general(inputs, grad_rows, (((0,), (0,)), ((), ())), preferred_element_type=jnp.float32)
            running = running + product
        mean_grad = running / N_DP
        new_first = beta_one * first_moment[layer_id] + (1.0 - beta_one) * mean_grad
        new_second = beta_two * second_moment[layer_id] + (1.0 - beta_two) * mean_grad * mean_grad
        update = new_first / correct_one / (jnp.sqrt(new_second / correct_two) + epsilon)
        firsts.append(new_first)
        seconds.append(new_second)
        updates.append(update)
    gain_grad = lax.optimization_barrier(jnp.sum(norm_grad.astype(jnp.float32) * normed.astype(jnp.float32), axis=1)) / N_DP
    return (jnp.stack(firsts), jnp.stack(seconds), jnp.stack(updates), gain_grad)
```

```python
import functools

import jax
import jax.numpy as jnp
from jax import lax
from jax.experimental import pallas as pl
from jax.experimental.pallas import tpu as pltpu
from jax.sharding import Mesh
from jax.sharding import PartitionSpec as P

AXES = ("x", "yl", "yh", "z", "c")
DP = ("x", "yl")
TP = ("yh", "z", "c")
DP_TP = AXES

beta_one = 0.9
beta_two = 0.95
correct_one = 0.19
correct_two = 0.0975
epsilon = 1e-08

F32 = jnp.float32
BF16 = jnp.bfloat16
VMEM = pl.BlockSpec(memory_space=pltpu.VMEM)
ANY = pl.BlockSpec(memory_space=pl.ANY)
STEPS = (0, -1, 1, -2, 2, -3, 3, 4)


def struct(shape, dtype):
    return jax.ShapeDtypeStruct(shape, dtype)


def cost(flops, bytes_moved):
    return pl.CostEstimate(flops=flops, bytes_accessed=bytes_moved, transcendentals=0)


def swap(array, axis, mask):
    size = lax.axis_size(axis)
    return lax.ppermute(array, axis, [(i, i ^ mask) for i in range(size)])


def shift(array, step):
    size = lax.axis_size("z")
    return lax.ppermute(array, "z", [(i, (i + step) % size) for i in range(size)])


def along_y(array, ab):
    if ab == 1:
        return swap(array, "yl", 1)
    if ab == 2:
        return swap(array, "yh", 1)
    return swap(array, ("yl", "yh"), 3)


def kernel_call(kernel, in_specs, out_shape, limit, estimate, operands, scratch=()):
    return pl.pallas_call(
        kernel,
        in_specs=in_specs,
        out_specs=[VMEM] * len(out_shape),
        out_shape=out_shape,
        scratch_shapes=list(scratch),
        cost_estimate=cost(*estimate),
        compiler_params=pltpu.CompilerParams(vmem_limit_bytes=limit << 20),
    )(*operands)


def order_kernel(k, rows_ref, *refs):
    out = refs[-1]
    x, yl = lax.axis_index("x"), lax.axis_index("yl")
    for j in range(4):
        for b in range(2):
            owner = (x ^ j) * 2 + (yl ^ b)
            to = (j * 2 + b) * 128
            start = pl.multiple_of(owner * 256 + k * 128, 128)
            out[:128, to : to + 128] = rows_ref[:, pl.ds(start, 128)]
    if k == 0:
        for q in range(8):
            sums = refs[0][q * 8 : (q + 1) * 8, :]
            high = sums.astype(BF16).astype(F32)
            out[128:144, q * 128 : (q + 1) * 128] = jnp.concatenate([high, sums - high]).astype(BF16)


def ordered(k, rows, gain):
    out = struct((144 if k == 0 else 128, 1024), BF16)
    specs = [VMEM] * (1 + len(gain))
    return kernel_call(functools.partial(order_kernel, k), specs, [out], 4, (1 << 20, 1 << 20), [rows, *gain])[0]


def turn_kernel(away, inputs_ref, out_ref):
    half, z, c = lax.axis_index("yh") ^ away, lax.axis_index("z"), lax.axis_index("c")
    for p, step in enumerate(STEPS):
        for own in range(2):
            start = half * 2048 + ((z + step + 8) % 8) * 256 + (c ^ own) * 128
            block = inputs_ref[pl.ds(pl.multiple_of(start, 128), 128), :]
            to = (p * 2 + own) * 128
            out_ref[:, to : to + 128] = block.T


def turned(inputs, away):
    return kernel_call(
        functools.partial(turn_kernel, away), [VMEM], [struct((256, 2048), BF16)], 6, (1 << 22, 2 << 20), [inputs]
    )[0]


def product_kernel(k, mine_ref, other_ref, *refs):
    blocks, outs = refs[:16], refs[16:24]
    rows, result, sems = refs[24:27]
    copies = [
        pltpu.make_async_copy(block.at[pl.ds(0, 128), :], rows.at[pl.ds(i * 128, 128), :], sems.at[i])
        for i, block in enumerate(blocks)
    ]
    if k == 0:
        gains, gain_sems = refs[27:]
        z, c = lax.axis_index("z"), lax.axis_index("c")
        for i, block in enumerate(blocks):
            source = ((z + STEPS[i // 2] + 8) % 8) * 2 + (c ^ (i % 2))
            copies.append(
                pltpu.make_async_copy(block.at[pl.ds(128, 16), :], gains.at[source], gain_sems.at[i])
            )
    for copy in copies:
        copy.start()
    for copy in copies:
        copy.wait()
    if k == 0:
        total = jnp.zeros((16, 1024), F32)
        for i in range(16):
            total = total + gains[i].astype(F32)
        total = total[:8] + total[8:]
        for q in range(8):
            at = slice(256 + (q % 4) * 8, 264 + (q % 4) * 8)
            to = slice((q // 4) * 128, (q // 4) * 128 + 128)
            for j in range(4):
                outs[j][at, to] = total[:, q * 128 : (q + 1) * 128]

    @pl.loop(0, 4)
    def _(j):
        start = pl.multiple_of(j * 256, 256)
        right = rows[:, pl.ds(start, 256)]
        result[:256, :] = jnp.dot(mine_ref[...], right, preferred_element_type=F32)
        result[256:, :] = jnp.dot(other_ref[...], right, preferred_element_type=F32)
        for at in range(4):

            @pl.when(j == at)
            def _():
                outs[at][:128, :] = result[:128, :]
                outs[at][128:256, :] = result[256:384, :]

        to = pl.multiple_of(j * 128, 128)
        for a in range(2):
            for b in range(2):
                outs[4 + a * 2 + b][:, pl.ds(to, 128)] = result[
                    a * 256 + 128 : a * 256 + 256, b * 128 : (b + 1) * 128
                ]


def product(k, mine, other, blocks):
    scratch = [pltpu.VMEM((2048, 1024), BF16), pltpu.VMEM((512, 256), F32), pltpu.SemaphoreType.DMA((16,))]
    if k == 0:
        scratch += [pltpu.VMEM((16, 16, 1024), BF16), pltpu.SemaphoreType.DMA((16,))]
    return kernel_call(
        functools.partial(product_kernel, k),
        [VMEM, VMEM] + [ANY] * 16,
        [struct((288 if k == 0 else 256, 256), F32)] * 4 + [struct((128, 512), F32)] * 4,
        14,
        (2 * 512 * 2048 * 1024, 8 << 20),
        [mine, other, *blocks],
        scratch,
    )


def sum_of(refs, at=slice(None)):
    own, one, two, three = (ref[at, :] for ref in refs)
    return (own + one) + (two + three)


def sum_rows_kernel(*refs):
    outs = refs[8:]
    for k in range(2):
        total = sum_of(refs[k * 4 : k * 4 + 4])
        for a in range(2):
            for b in range(2):
                outs[a * 2 + b][:128, k * 128 : (k + 1) * 128] = total[
                    a * 128 : (a + 1) * 128, b * 128 : (b + 1) * 128
                ]
        if k == 0:
            for out in outs:
                out[128:160, :] = total[256:288, :]


def sum_columns_kernel(*refs):
    outs = refs[8:]
    for k in range(2):
        total = sum_of(refs[k * 4 : k * 4 + 4])
        for j in range(4):
            outs[j][:, k * 128 : (k + 1) * 128] = total[:, j * 128 : (j + 1) * 128]


def cut_sum(kernel, parts, rows):
    return kernel_call(kernel, [VMEM] * 8, [struct((rows, 256), F32)] * 4, 5, (1 << 18, 1 << 20), parts)


def adam_kernel(scale, first_ref, second_ref, *refs):
    pieces, (new_first_ref, new_second_ref, update_ref, gain_ref) = refs[:8], refs[8:]
    gain = sum_of(pieces[:4], slice(128, 160)) * scale
    gain_ref[:32, :] = gain[:, :128]
    gain_ref[32:, :] = gain[:, 128:]
    for r in range(2):
        grad = sum_of(pieces[r * 4 : r * 4 + 4], slice(0, 128)) * scale
        at = (slice(r * 128, (r + 1) * 128), slice(None))
        new_first = beta_one * first_ref[at] + (1.0 - beta_one) * grad
        new_second = beta_two * second_ref[at] + (1.0 - beta_two) * grad * grad
        new_first_ref[at] = new_first
        new_second_ref[at] = new_second
        update_ref[at] = new_first / correct_one / (jnp.sqrt(new_second / correct_two) + epsilon)


def adam(scale, first_old, second_old, pieces):
    return kernel_call(
        functools.partial(adam_kernel, scale),
        [VMEM] * 10,
        [struct((256, 256), F32)] * 3 + [struct((64, 128), F32)],
        5,
        (1 << 20, 2 << 20),
        [first_old, second_old, *pieces],
    )


def shards(proj_in, kv_grad, normed, norm_grad, first_moment, second_moment):
    return update_of(proj_in[0], kv_grad[0], normed, norm_grad, first_moment[0], second_moment[0])


def update_of(inputs, rows, normed, norm_grad, first_moment, second_moment):
    replicas = lax.axis_size(DP)
    gain = jnp.sum(norm_grad.astype(F32) * normed.astype(F32), axis=1).reshape(64, 128)
    starts = [ordered(0, rows, [gain]), ordered(1, rows, [])]

    def gathered(k):
        own = {0: starts[k]}
        up = down = starts[k]
        for step in (1, 2, 3, 4):
            if step < 4 or k == 0:
                up = shift(up, 1)
                own[4 if step == 4 else -step] = up
            if step < 4 or k == 1:
                down = shift(down, -1)
                own[step] = down
        blocks = []
        for step in STEPS:
            blocks += [own[step], swap(own[step], "c", 1)]
        return blocks

    gathers = [gathered(k) for k in range(2)]
    mine = turned(inputs, 0)
    other = swap(turned(inputs, 1), "yh", 1)

    in_x, in_y = [], []
    for k in range(2):
        outs = product(k, mine, other, gathers[k])
        by_x, by_y = outs[:4], outs[4:]
        in_x += [by_x[0]] + [swap(by_x[j], "x", j) for j in (1, 2, 3)]
        in_y += [by_y[0]] + [along_y(by_y[ab], ab) for ab in (1, 2, 3)]
    by_y = cut_sum(sum_rows_kernel, in_x, 160)
    by_x = cut_sum(sum_columns_kernel, in_y, 128)
    pieces = [by_y[0]] + [along_y(by_y[ab], ab) for ab in (1, 2, 3)]
    pieces += [by_x[0]] + [swap(by_x[j], "x", j) for j in (1, 2, 3)]
    new_first, new_second, update, gain = adam(1.0 / replicas, first_moment, second_moment, pieces)
    return (new_first[None], new_second[None], update[None], gain.reshape(1, 8192))


def solution(mesh):
    finer = Mesh(mesh.devices.reshape(4, 2, 2, 8, 2), AXES)
    return jax.shard_map(
        shards,
        mesh=finer,
        in_specs=(
            P(None, DP, TP),
            P(None, DP_TP, None),
            P(None, DP_TP, None),
            P(None, DP_TP, None),
            P(None, TP, DP),
            P(None, TP, DP),
        ),
        out_specs=(P(None, TP, DP), P(None, TP, DP), P(None, TP, DP), P()),
        check_vma=False,
    )
```

```python
import functools

import jax
import jax.numpy as jnp
from jax import lax
from jax.experimental import pallas as pl
from jax.experimental.pallas import tpu as pltpu
from jax.sharding import Mesh
from jax.sharding import PartitionSpec as P

AXES = ("x", "yl", "yh", "z", "c")
DP = ("x", "yl")
TP = ("yh", "z", "c")
DP_TP = AXES

beta_one = 0.9
beta_two = 0.95
correct_one = 0.19
correct_two = 0.0975
epsilon = 1e-08

F32 = jnp.float32
BF16 = jnp.bfloat16
VMEM = pl.BlockSpec(memory_space=pltpu.VMEM)
ANY = pl.BlockSpec(memory_space=pl.ANY)
STEPS = (0, -1, 1, -2, 2, -3, 3, 4)


def struct(shape, dtype):
    return jax.ShapeDtypeStruct(shape, dtype)


def cost(flops, bytes_moved):
    return pl.CostEstimate(flops=flops, bytes_accessed=bytes_moved, transcendentals=0)


def swap(array, axis, mask):
    size = lax.axis_size(axis)
    return lax.ppermute(array, axis, [(i, i ^ mask) for i in range(size)])


def shift(array, step):
    size = lax.axis_size("z")
    return lax.ppermute(array, "z", [(i, (i + step) % size) for i in range(size)])


def along_y(array, ab):
    if ab == 1:
        return swap(array, "yl", 1)
    if ab == 2:
        return swap(array, "yh", 1)
    return swap(array, ("yl", "yh"), 3)


def kernel_call(kernel, in_specs, out_shape, limit, estimate, operands, scratch=()):
    return pl.pallas_call(
        kernel,
        in_specs=in_specs,
        out_specs=[VMEM] * len(out_shape),
        out_shape=out_shape,
        scratch_shapes=list(scratch),
        cost_estimate=cost(*estimate),
        compiler_params=pltpu.CompilerParams(vmem_limit_bytes=limit << 20),
    )(*operands)


def order_kernel(k, rows_ref, *refs):
    out = refs[-1]
    x, yl = lax.axis_index("x"), lax.axis_index("yl")
    for j in range(4):
        for b in range(2):
            owner = (x ^ j) * 2 + (yl ^ b)
            to = (j * 2 + b) * 128
            start = pl.multiple_of(owner * 256 + k * 128, 128)
            out[:128, to : to + 128] = rows_ref[:, pl.ds(start, 128)]
    if k == 0:
        for q in range(8):
            sums = refs[0][q * 8 : (q + 1) * 8, :]
            high = sums.astype(BF16).astype(F32)
            out[128:144, q * 128 : (q + 1) * 128] = jnp.concatenate([high, sums - high]).astype(BF16)


def ordered(k, rows, gain):
    out = struct((144 if k == 0 else 128, 1024), BF16)
    specs = [VMEM] * (1 + len(gain))
    return kernel_call(
        functools.partial(order_kernel, k), specs, [out], 4, (1 << 20, 1 << 20), [rows, *gain]
    )[0]


def turn_kernel(away, inputs_ref, out_ref):
    half, z, c = lax.axis_index("yh") ^ away, lax.axis_index("z"), lax.axis_index("c")
    for p, step in enumerate(STEPS):
        for own in range(2):
            start = half * 2048 + ((z + step + 8) % 8) * 256 + (c ^ own) * 128
            block = inputs_ref[pl.ds(pl.multiple_of(start, 128), 128), :]
            to = (p * 2 + own) * 128
            out_ref[:, to : to + 128] = block.T


def turned(inputs, away):
    return kernel_call(
        functools.partial(turn_kernel, away),
        [VMEM],
        [struct((256, 2048), BF16)],
        6,
        (1 << 22, 2 << 20),
        [inputs],
    )[0]


def product_kernel(k, mine_ref, other_ref, *refs):
    blocks, outs = refs[:16], refs[16:24]
    rows, result, sems = refs[24:27]

    def copies_of(j):
        columns = pl.ds(pl.multiple_of(j * 256, 256), 256)
        return [
            pltpu.make_async_copy(
                block.at[pl.ds(0, 128), columns], rows.at[j, pl.ds(i * 128, 128), :], sems.at[j, i]
            )
            for i, block in enumerate(blocks)
        ]

    @pl.loop(0, 4)
    def _(j):
        for copy in copies_of(j):
            copy.start()

    gain_copies = []
    if k == 0:
        gains, gain_sems = refs[27:]
        z, c = lax.axis_index("z"), lax.axis_index("c")
        for i, block in enumerate(blocks):
            source = ((z + STEPS[i // 2] + 8) % 8) * 2 + (c ^ (i % 2))
            gain_copies.append(
                pltpu.make_async_copy(block.at[pl.ds(128, 16), :], gains.at[source], gain_sems.at[i])
            )
    for copy in gain_copies:
        copy.start()

    @pl.loop(0, 4)
    def _(j):
        for copy in copies_of(j):
            copy.wait()
        right = rows[j]
        result[:256, :] = jnp.dot(mine_ref[...], right, preferred_element_type=F32)
        result[256:, :] = jnp.dot(other_ref[...], right, preferred_element_type=F32)
        for at in range(4):

            @pl.when(j == at)
            def _():
                outs[at][:128, :] = result[:128, :]
                outs[at][128:256, :] = result[256:384, :]

        to = pl.multiple_of(j * 128, 128)
        for a in range(2):
            for b in range(2):
                outs[4 + a * 2 + b][:, pl.ds(to, 128)] = result[
                    a * 256 + 128 : a * 256 + 256, b * 128 : (b + 1) * 128
                ]

    for copy in gain_copies:
        copy.wait()
    if k == 0:
        total = jnp.zeros((16, 1024), F32)
        for i in range(16):
            total = total + gains[i].astype(F32)
        total = total[:8] + total[8:]
        for q in range(8):
            at = slice(256 + (q % 4) * 8, 264 + (q % 4) * 8)
            to = slice((q // 4) * 128, (q // 4) * 128 + 128)
            for j in range(4):
                outs[j][at, to] = total[:, q * 128 : (q + 1) * 128]


def product(k, mine, other, blocks):
    scratch = [pltpu.VMEM((4, 2048, 256), BF16), pltpu.VMEM((512, 256), F32), pltpu.SemaphoreType.DMA((4, 16))]
    if k == 0:
        scratch += [pltpu.VMEM((16, 16, 1024), BF16), pltpu.SemaphoreType.DMA((16,))]
    return kernel_call(
        functools.partial(product_kernel, k),
        [VMEM, VMEM] + [ANY] * 16,
        [struct((288 if k == 0 else 256, 256), F32)] * 4 + [struct((128, 512), F32)] * 4,
        14,
        (2 * 512 * 2048 * 1024, 8 << 20),
        [mine, other, *blocks],
        scratch,
    )


def sum_of(refs, at=slice(None)):
    own, one, two, three = (ref[at, :] for ref in refs)
    return (own + one) + (two + three)


def sum_rows_kernel(*refs):
    outs = refs[8:]
    for k in range(2):
        total = sum_of(refs[k * 4 : k * 4 + 4])
        for a in range(2):
            for b in range(2):
                outs[a * 2 + b][:128, k * 128 : (k + 1) * 128] = total[
                    a * 128 : (a + 1) * 128, b * 128 : (b + 1) * 128
                ]
        if k == 0:
            for out in outs:
                out[128:160, :] = total[256:288, :]


def sum_columns_kernel(*refs):
    outs = refs[8:]
    for k in range(2):
        total = sum_of(refs[k * 4 : k * 4 + 4])
        for j in range(4):
            outs[j][:, k * 128 : (k + 1) * 128] = total[:, j * 128 : (j + 1) * 128]


def cut_sum(kernel, parts, rows):
    return kernel_call(
        kernel, [VMEM] * 8, [struct((rows, 256), F32)] * 4, 5, (1 << 18, 1 << 20), parts
    )


def adam_kernel(scale, first_ref, second_ref, *refs):
    pieces, (new_first_ref, new_second_ref, update_ref, gain_ref) = refs[:8], refs[8:]
    gain = sum_of(pieces[:4], slice(128, 160)) * scale
    gain_ref[:32, :] = gain[:, :128]
    gain_ref[32:, :] = gain[:, 128:]
    for r in range(2):
        grad = sum_of(pieces[r * 4 : r * 4 + 4], slice(0, 128)) * scale
        at = (slice(r * 128, (r + 1) * 128), slice(None))
        new_first = beta_one * first_ref[at] + (1.0 - beta_one) * grad
        new_second = beta_two * second_ref[at] + (1.0 - beta_two) * grad * grad
        new_first_ref[at] = new_first
        new_second_ref[at] = new_second
        update_ref[at] = new_first / correct_one / (jnp.sqrt(new_second / correct_two) + epsilon)


def adam(scale, first_old, second_old, pieces):
    return kernel_call(
        functools.partial(adam_kernel, scale),
        [VMEM] * 10,
        [struct((256, 256), F32)] * 3 + [struct((64, 128), F32)],
        5,
        (1 << 20, 2 << 20),
        [first_old, second_old, *pieces],
    )


def shards(proj_in, kv_grad, normed, norm_grad, first_moment, second_moment):
    return update_of(proj_in[0], kv_grad[0], normed, norm_grad, first_moment[0], second_moment[0])


def update_of(inputs, rows, normed, norm_grad, first_moment, second_moment):
    replicas = lax.axis_size(DP)
    gain = jnp.sum(norm_grad.astype(F32) * normed.astype(F32), axis=1).reshape(64, 128)
    starts = [ordered(0, rows, [gain]), ordered(1, rows, [])]

    def gathered(k):
        own = {0: starts[k]}
        up = down = starts[k]
        for step in (1, 2, 3, 4):
            if step < 4 or k == 0:
                up = shift(up, 1)
                own[4 if step == 4 else -step] = up
            if step < 4 or k == 1:
                down = shift(down, -1)
                own[step] = down
        blocks = []
        for step in STEPS:
            blocks += [own[step], swap(own[step], "c", 1)]
        return blocks

    gathers = [gathered(k) for k in range(2)]
    mine = turned(inputs, 0)
    other = swap(turned(inputs, 1), "yh", 1)

    in_x, in_y = [], []
    for k in range(2):
        outs = product(k, mine, other, gathers[k])
        by_x, by_y = outs[:4], outs[4:]
        in_x += [by_x[0]] + [swap(by_x[j], "x", j) for j in (1, 2, 3)]
        in_y += [by_y[0]] + [along_y(by_y[ab], ab) for ab in (1, 2, 3)]
    by_y = cut_sum(sum_rows_kernel, in_x, 160)
    by_x = cut_sum(sum_columns_kernel, in_y, 128)
    pieces = [by_y[0]] + [along_y(by_y[ab], ab) for ab in (1, 2, 3)]
    pieces += [by_x[0]] + [swap(by_x[j], "x", j) for j in (1, 2, 3)]
    new_first, new_second, update, gain = adam(1.0 / replicas, first_moment, second_moment, pieces)
    return (new_first[None], new_second[None], update[None], gain.reshape(1, 8192))


def solution(mesh):
    finer = Mesh(mesh.devices.reshape(4, 2, 2, 8, 2), AXES)
    return jax.shard_map(
        shards,
        mesh=finer,
        in_specs=(
            P(None, DP, TP),
            P(None, DP_TP, None),
            P(None, DP_TP, None),
            P(None, DP_TP, None),
            P(None, TP, DP),
            P(None, TP, DP),
        ),
        out_specs=(P(None, TP, DP), P(None, TP, DP), P(None, TP, DP), P()),
        check_vma=False,
    )
```

```python
import functools

import jax
import jax.numpy as jnp
from jax import lax
from jax.experimental import pallas as pl
from jax.experimental.pallas import tpu as pltpu
from jax.sharding import Mesh
from jax.sharding import PartitionSpec as P

AXES = ("x", "yl", "yh", "z", "c")
DP = ("x", "yl")
TP = ("yh", "z", "c")
DP_TP = AXES

beta_one = 0.9
beta_two = 0.95
correct_one = 0.19
correct_two = 0.0975
epsilon = 1e-08

F32 = jnp.float32
BF16 = jnp.bfloat16
VMEM = pl.BlockSpec(memory_space=pltpu.VMEM)
ANY = pl.BlockSpec(memory_space=pl.ANY)
STEPS = (0, -1, 1, -2, 2, -3, 3, 4)


def struct(shape, dtype):
    return jax.ShapeDtypeStruct(shape, dtype)


def cost(flops, bytes_moved):
    return pl.CostEstimate(flops=flops, bytes_accessed=bytes_moved, transcendentals=0)


def swap(array, axis, mask):
    size = lax.axis_size(axis)
    return lax.ppermute(array, axis, [(i, i ^ mask) for i in range(size)])


def shift(array, step):
    size = lax.axis_size("z")
    return lax.ppermute(array, "z", [(i, (i + step) % size) for i in range(size)])


def along_y(array, ab):
    if ab == 1:
        return swap(array, "yl", 1)
    if ab == 2:
        return swap(array, "yh", 1)
    return swap(array, ("yl", "yh"), 3)


def kernel_call(kernel, in_specs, out_shape, limit, estimate, operands, scratch=()):
    return pl.pallas_call(
        kernel,
        in_specs=in_specs,
        out_specs=[VMEM] * len(out_shape),
        out_shape=out_shape,
        scratch_shapes=list(scratch),
        cost_estimate=cost(*estimate),
        compiler_params=pltpu.CompilerParams(vmem_limit_bytes=limit << 20),
    )(*operands)


def order_kernel(k, rows_ref, *refs):
    out = refs[-1]
    x, yl = lax.axis_index("x"), lax.axis_index("yl")
    for j in range(4):
        for b in range(2):
            owner = (x ^ j) * 2 + (yl ^ b)
            to = (j * 2 + b) * 128
            start = pl.multiple_of(owner * 256 + k * 128, 128)
            out[:128, to : to + 128] = rows_ref[:, pl.ds(start, 128)]
    if k == 0:
        for q in range(8):
            sums = refs[0][q * 8 : (q + 1) * 8, :]
            high = sums.astype(BF16).astype(F32)
            out[128:144, q * 128 : (q + 1) * 128] = jnp.concatenate([high, sums - high]).astype(BF16)


def ordered(k, rows, gain):
    out = struct((144 if k == 0 else 128, 1024), BF16)
    specs = [VMEM] * (1 + len(gain))
    return kernel_call(functools.partial(order_kernel, k), specs, [out], 4, (1 << 20, 1 << 20), [rows, *gain])[0]


def turn_kernel(away, inputs_ref, out_ref):
    half, z, c = lax.axis_index("yh") ^ away, lax.axis_index("z"), lax.axis_index("c")
    for p, step in enumerate(STEPS):
        for own in range(2):
            start = half * 2048 + ((z + step + 8) % 8) * 256 + (c ^ own) * 128
            block = inputs_ref[pl.ds(pl.multiple_of(start, 128), 128), :]
            to = (p * 2 + own) * 128
            out_ref[:, to : to + 128] = block.T


def turned(inputs, away):
    return kernel_call(
        functools.partial(turn_kernel, away), [VMEM], [struct((256, 2048), BF16)], 6, (1 << 22, 2 << 20), [inputs]
    )[0]


def part_kernel(k, mine_ref, other_ref, *refs):
    blocks, outs, refs = refs[:14], refs[14:22], refs[22:]
    if k == 0:
        gains_ref, refs = refs[0], refs[1:]
    rows, result, sems = refs[:3]
    copies = [
        pltpu.make_async_copy(block.at[pl.ds(0, 128), :], rows.at[pl.ds(i * 128, 128), :], sems.at[i])
        for i, block in enumerate(blocks)
    ]
    if k == 0:
        for i, block in enumerate(blocks):
            copies.append(
                pltpu.make_async_copy(block.at[pl.ds(128, 16), :], gains_ref.at[source_of(i)], refs[3].at[i])
            )
    for copy in copies:
        copy.start()
    for copy in copies:
        copy.wait()

    @pl.loop(0, 4)
    def _(j):
        right = rows[:, pl.ds(pl.multiple_of(j * 256, 256), 256)]
        result[:256, :] = jnp.dot(mine_ref[:, :1792], right, preferred_element_type=F32)
        result[256:, :] = jnp.dot(other_ref[:, :1792], right, preferred_element_type=F32)
        for at in range(4):

            @pl.when(j == at)
            def _():
                outs[at][:128, :] = result[:128, :]
                outs[at][128:256, :] = result[256:384, :]

        to = pl.multiple_of(j * 128, 128)
        for a in range(2):
            for b in range(2):
                outs[4 + a * 2 + b][:, pl.ds(to, 128)] = result[
                    a * 256 + 128 : a * 256 + 256, b * 128 : (b + 1) * 128
                ]


def source_of(i):
    z, c = lax.axis_index("z"), lax.axis_index("c")
    return ((z + STEPS[i // 2] + 8) % 8) * 2 + (c ^ (i % 2))


def product_kernel(k, mine_ref, other_ref, own_ref, swapped_ref, *refs):
    parts, refs = refs[:8], refs[8:]
    if k == 0:
        gains_ref, refs = refs[0], refs[1:]
    outs = refs
    for j in range(4):
        columns = slice(j * 256, (j + 1) * 256)
        right = jnp.concatenate([own_ref[:128, columns], swapped_ref[:128, columns]], axis=0)
        for a, left in enumerate((mine_ref, other_ref)):
            result = jnp.dot(left[:, 1792:], right, preferred_element_type=F32)
            at = slice(a * 128, (a + 1) * 128)
            outs[j][at, :] = parts[j][at, :] + result[:128]
            for b in range(2):
                to = slice(j * 128, (j + 1) * 128)
                piece = 4 + a * 2 + b
                outs[piece][:, to] = parts[piece][:, to] + result[128:, b * 128 : (b + 1) * 128]
    if k == 0:
        late = [(source_of(14), own_ref[128:144, :].astype(F32)), (source_of(15), swapped_ref[128:144, :].astype(F32))]
        total = jnp.zeros((16, 1024), F32)
        for i in range(16):
            value = gains_ref[i].astype(F32)
            for source, here in late:
                value = jnp.where(source == i, here, value)
            total = total + value
        total = total[:8] + total[8:]
        for q in range(8):
            at = slice(256 + (q % 4) * 8, 264 + (q % 4) * 8)
            to = slice((q // 4) * 128, (q // 4) * 128 + 128)
            for j in range(4):
                outs[j][at, to] = total[:, q * 128 : (q + 1) * 128]


def product(k, mine, other, blocks):
    pieces = [struct((128, 512), F32)] * 4
    scratch = [pltpu.VMEM((1792, 1024), BF16), pltpu.VMEM((512, 256), F32), pltpu.SemaphoreType.DMA((14,))]
    gains = []
    if k == 0:
        scratch += [pltpu.SemaphoreType.DMA((14,))]
        gains = [struct((16, 16, 1024), BF16)]
    parts = kernel_call(
        functools.partial(part_kernel, k),
        [VMEM, VMEM] + [ANY] * 14,
        [struct((256, 256), F32)] * 4 + pieces + gains,
        14,
        (2 * 512 * 1792 * 1024, 8 << 20),
        [mine, other, *blocks[:14]],
        scratch,
    )
    return kernel_call(
        functools.partial(product_kernel, k),
        [VMEM] * (4 + len(parts)),
        [struct((288 if k == 0 else 256, 256), F32)] * 4 + pieces,
        14,
        (2 * 512 * 256 * 1024, 4 << 20),
        [mine, other, *blocks[14:], *parts],
    )


def sum_of(refs, at=slice(None)):
    own, one, two, three = (ref[at, :] for ref in refs)
    return (own + one) + (two + three)


def sum_rows_kernel(*refs):
    outs = refs[8:]
    for k in range(2):
        total = sum_of(refs[k * 4 : k * 4 + 4])
        for a in range(2):
            for b in range(2):
                outs[a * 2 + b][:128, k * 128 : (k + 1) * 128] = total[
                    a * 128 : (a + 1) * 128, b * 128 : (b + 1) * 128
                ]
        if k == 0:
            for out in outs:
                out[128:160, :] = total[256:288, :]


def sum_columns_kernel(*refs):
    outs = refs[8:]
    for k in range(2):
        total = sum_of(refs[k * 4 : k * 4 + 4])
        for j in range(4):
            outs[j][:, k * 128 : (k + 1) * 128] = total[:, j * 128 : (j + 1) * 128]


def cut_sum(kernel, parts, rows):
    return kernel_call(kernel, [VMEM] * 8, [struct((rows, 256), F32)] * 4, 5, (1 << 18, 1 << 20), parts)


def adam_kernel(scale, first_ref, second_ref, *refs):
    pieces, (new_first_ref, new_second_ref, update_ref, gain_ref) = refs[:8], refs[8:]
    gain = sum_of(pieces[:4], slice(128, 160)) * scale
    gain_ref[:32, :] = gain[:, :128]
    gain_ref[32:, :] = gain[:, 128:]
    for r in range(2):
        grad = sum_of(pieces[r * 4 : r * 4 + 4], slice(0, 128)) * scale
        at = (slice(r * 128, (r + 1) * 128), slice(None))
        new_first = beta_one * first_ref[at] + (1.0 - beta_one) * grad
        new_second = beta_two * second_ref[at] + (1.0 - beta_two) * grad * grad
        new_first_ref[at] = new_first
        new_second_ref[at] = new_second
        update_ref[at] = new_first / correct_one / (jnp.sqrt(new_second / correct_two) + epsilon)


def adam(scale, first_old, second_old, pieces):
    return kernel_call(
        functools.partial(adam_kernel, scale),
        [VMEM] * 10,
        [struct((256, 256), F32)] * 3 + [struct((64, 128), F32)],
        5,
        (1 << 20, 2 << 20),
        [first_old, second_old, *pieces],
    )


def shards(proj_in, kv_grad, normed, norm_grad, first_moment, second_moment):
    return update_of(proj_in[0], kv_grad[0], normed, norm_grad, first_moment[0], second_moment[0])


def update_of(inputs, rows, normed, norm_grad, first_moment, second_moment):
    replicas = lax.axis_size(DP)
    gain = jnp.sum(norm_grad.astype(F32) * normed.astype(F32), axis=1).reshape(64, 128)
    starts = [ordered(0, rows, [gain]), ordered(1, rows, [])]

    def gathered(k):
        own = {0: starts[k]}
        up = down = starts[k]
        for step in (1, 2, 3, 4):
            if step < 4 or k == 0:
                up = shift(up, 1)
                own[4 if step == 4 else -step] = up
            if step < 4 or k == 1:
                down = shift(down, -1)
                own[step] = down
        blocks = []
        for step in STEPS:
            blocks += [own[step], swap(own[step], "c", 1)]
        return blocks

    gathers = [gathered(k) for k in range(2)]
    mine = turned(inputs, 0)
    other = swap(turned(inputs, 1), "yh", 1)

    in_x, in_y = [], []
    for k in range(2):
        outs = product(k, mine, other, gathers[k])
        by_x, by_y = outs[:4], outs[4:]
        in_x += [by_x[0]] + [swap(by_x[j], "x", j) for j in (1, 2, 3)]
        in_y += [by_y[0]] + [along_y(by_y[ab], ab) for ab in (1, 2, 3)]
    by_y = cut_sum(sum_rows_kernel, in_x, 160)
    by_x = cut_sum(sum_columns_kernel, in_y, 128)
    pieces = [by_y[0]] + [along_y(by_y[ab], ab) for ab in (1, 2, 3)]
    pieces += [by_x[0]] + [swap(by_x[j], "x", j) for j in (1, 2, 3)]
    new_first, new_second, update, gain = adam(1.0 / replicas, first_moment, second_moment, pieces)
    return (new_first[None], new_second[None], update[None], gain.reshape(1, 8192))


def solution(mesh):
    finer = Mesh(mesh.devices.reshape(4, 2, 2, 8, 2), AXES)
    return jax.shard_map(
        shards,
        mesh=finer,
        in_specs=(
            P(None, DP, TP),
            P(None, DP_TP, None),
            P(None, DP_TP, None),
            P(None, DP_TP, None),
            P(None, TP, DP),
            P(None, TP, DP),
        ),
        out_specs=(P(None, TP, DP), P(None, TP, DP), P(None, TP, DP), P()),
        check_vma=False,
    )
```

```python
import functools

import jax
import jax.numpy as jnp
from jax import lax
from jax.experimental import pallas as pl
from jax.experimental.pallas import tpu as pltpu
from jax.sharding import Mesh
from jax.sharding import PartitionSpec as P

AXES = ("x", "yl", "yh", "z", "c")
DP = ("x", "yl")
TP = ("yh", "z", "c")
DP_TP = AXES

beta_one = 0.9
beta_two = 0.95
correct_one = 0.19
correct_two = 0.0975
epsilon = 1e-08

F32 = jnp.float32
BF16 = jnp.bfloat16
VMEM = pl.BlockSpec(memory_space=pltpu.VMEM)
STEPS = (0, -1, 1, -2, 2, -3, 3, 4)


def struct(shape, dtype):
    return jax.ShapeDtypeStruct(shape, dtype)


def cost(flops, bytes_moved):
    return pl.CostEstimate(flops=flops, bytes_accessed=bytes_moved, transcendentals=0)


def swap(array, axis, mask):
    size = lax.axis_size(axis)
    return lax.ppermute(array, axis, [(i, i ^ mask) for i in range(size)])


def shift(array, step):
    size = lax.axis_size("z")
    return lax.ppermute(array, "z", [(i, (i + step) % size) for i in range(size)])


def along_y(array, ab):
    if ab == 1:
        return swap(array, "yl", 1)
    if ab == 2:
        return swap(array, "yh", 1)
    return swap(array, ("yl", "yh"), 3)


def kernel_call(kernel, in_specs, out_shape, limit, estimate, operands, scratch=()):
    return pl.pallas_call(
        kernel,
        in_specs=in_specs,
        out_specs=[VMEM] * len(out_shape),
        out_shape=out_shape,
        scratch_shapes=list(scratch),
        cost_estimate=cost(*estimate),
        compiler_params=pltpu.CompilerParams(vmem_limit_bytes=limit << 20),
    )(*operands)


def order_kernel(k, rows_ref, *refs):
    out = refs[-1]
    x, yl = lax.axis_index("x"), lax.axis_index("yl")
    for j in range(4):
        for b in range(2):
            owner = (x ^ j) * 2 + (yl ^ b)
            to = (j * 2 + b) * 128
            start = pl.multiple_of(owner * 256 + k * 128, 128)
            out[:128, to : to + 128] = rows_ref[:, pl.ds(start, 128)]
    if k == 0:
        for q in range(8):
            sums = refs[0][q * 8 : (q + 1) * 8, :]
            high = sums.astype(BF16).astype(F32)
            out[128:144, q * 128 : (q + 1) * 128] = jnp.concatenate([high, sums - high]).astype(BF16)


def ordered(k, rows, gain):
    out = struct((144 if k == 0 else 128, 1024), BF16)
    specs = [VMEM] * (1 + len(gain))
    return kernel_call(
        functools.partial(order_kernel, k), specs, [out], 4, (1 << 20, 1 << 20), [rows, *gain]
    )[0]


def turn_kernel(away, inputs_ref, out_ref):
    half, z, c = lax.axis_index("yh") ^ away, lax.axis_index("z"), lax.axis_index("c")
    for p, step in enumerate(STEPS):
        for own in range(2):
            start = half * 2048 + ((z + step + 8) % 8) * 256 + (c ^ own) * 128
            block = inputs_ref[pl.ds(pl.multiple_of(start, 128), 128), :]
            to = (p * 2 + own) * 128
            out_ref[:, to : to + 128] = block.T


def turned(inputs, away):
    return kernel_call(
        functools.partial(turn_kernel, away),
        [VMEM],
        [struct((256, 2048), BF16)],
        6,
        (1 << 22, 2 << 20),
        [inputs],
    )[0]


def part_kernel(k, mine_ref, other_ref, *refs):
    blocks, outs, refs = refs[:14], refs[14:22], refs[22:]
    if k == 0:
        gains_ref, refs = refs[0], refs[1:]
        for i, block in enumerate(blocks):
            gains_ref[source_of(i)] = block[128:144, :]
    rows, result = refs

    @pl.loop(0, 4)
    def _(j):
        columns = pl.ds(pl.multiple_of(j * 256, 256), 256)
        for i, block in enumerate(blocks):
            rows[i * 128 : (i + 1) * 128, :] = block[:128, columns]
        right = rows[...]
        result[:256, :] = jnp.dot(mine_ref[:, :1792], right, preferred_element_type=F32)
        result[256:, :] = jnp.dot(other_ref[:, :1792], right, preferred_element_type=F32)
        for at in range(4):

            @pl.when(j == at)
            def _():
                outs[at][:128, :] = result[:128, :]
                outs[at][128:256, :] = result[256:384, :]

        to = pl.multiple_of(j * 128, 128)
        for a in range(2):
            for b in range(2):
                outs[4 + a * 2 + b][:, pl.ds(to, 128)] = result[
                    a * 256 + 128 : a * 256 + 256, b * 128 : (b + 1) * 128
                ]


def source_of(i):
    z, c = lax.axis_index("z"), lax.axis_index("c")
    return ((z + STEPS[i // 2] + 8) % 8) * 2 + (c ^ (i % 2))


def product_kernel(k, mine_ref, other_ref, own_ref, swapped_ref, *refs):
    parts, refs = refs[:8], refs[8:]
    if k == 0:
        gains_ref, refs = refs[0], refs[1:]
    outs = refs
    for j in range(4):
        columns = slice(j * 256, (j + 1) * 256)
        right = jnp.concatenate([own_ref[:128, columns], swapped_ref[:128, columns]], axis=0)
        for a, left in enumerate((mine_ref, other_ref)):
            result = jnp.dot(left[:, 1792:], right, preferred_element_type=F32)
            at = slice(a * 128, (a + 1) * 128)
            outs[j][at, :] = parts[j][at, :] + result[:128]
            for b in range(2):
                to = slice(j * 128, (j + 1) * 128)
                piece = 4 + a * 2 + b
                outs[piece][:, to] = parts[piece][:, to] + result[128:, b * 128 : (b + 1) * 128]
    if k == 0:
        late = [(source_of(14), own_ref[128:144, :].astype(F32)), (source_of(15), swapped_ref[128:144, :].astype(F32))]
        total = jnp.zeros((16, 1024), F32)
        for i in range(16):
            value = gains_ref[i].astype(F32)
            for source, here in late:
                value = jnp.where(source == i, here, value)
            total = total + value
        total = total[:8] + total[8:]
        for q in range(8):
            at = slice(256 + (q % 4) * 8, 264 + (q % 4) * 8)
            to = slice((q // 4) * 128, (q // 4) * 128 + 128)
            for j in range(4):
                outs[j][at, to] = total[:, q * 128 : (q + 1) * 128]


def product(k, mine, other, blocks):
    pieces = [struct((128, 512), F32)] * 4
    scratch = [pltpu.VMEM((1792, 256), BF16), pltpu.VMEM((512, 256), F32)]
    gains = [struct((16, 16, 1024), BF16)] if k == 0 else []
    parts = kernel_call(
        functools.partial(part_kernel, k),
        [VMEM] * 16,
        [struct((256, 256), F32)] * 4 + pieces + gains,
        14,
        (2 * 512 * 1792 * 1024, 8 << 20),
        [mine, other, *blocks[:14]],
        scratch,
    )
    return kernel_call(
        functools.partial(product_kernel, k),
        [VMEM] * (4 + len(parts)),
        [struct((288 if k == 0 else 256, 256), F32)] * 4 + pieces,
        14,
        (2 * 512 * 256 * 1024, 4 << 20),
        [mine, other, *blocks[14:], *parts],
    )


def sum_of(refs, at=slice(None)):
    own, one, two, three = (ref[at, :] for ref in refs)
    return (own + one) + (two + three)


def sum_rows_kernel(*refs):
    outs = refs[8:]
    for k in range(2):
        total = sum_of(refs[k * 4 : k * 4 + 4])
        for a in range(2):
            for b in range(2):
                outs[a * 2 + b][:128, k * 128 : (k + 1) * 128] = total[
                    a * 128 : (a + 1) * 128, b * 128 : (b + 1) * 128
                ]
        if k == 0:
            for out in outs:
                out[128:160, :] = total[256:288, :]


def sum_columns_kernel(*refs):
    outs = refs[8:]
    for k in range(2):
        total = sum_of(refs[k * 4 : k * 4 + 4])
        for j in range(4):
            outs[j][:, k * 128 : (k + 1) * 128] = total[:, j * 128 : (j + 1) * 128]


def cut_sum(kernel, parts, rows):
    return kernel_call(
        kernel, [VMEM] * 8, [struct((rows, 256), F32)] * 4, 5, (1 << 18, 1 << 20), parts
    )


def adam_kernel(scale, first_ref, second_ref, *refs):
    pieces, (new_first_ref, new_second_ref, update_ref, gain_ref) = refs[:8], refs[8:]
    gain = sum_of(pieces[:4], slice(128, 160)) * scale
    gain_ref[:32, :] = gain[:, :128]
    gain_ref[32:, :] = gain[:, 128:]
    for r in range(2):
        grad = sum_of(pieces[r * 4 : r * 4 + 4], slice(0, 128)) * scale
        at = (slice(r * 128, (r + 1) * 128), slice(None))
        new_first = beta_one * first_ref[at] + (1.0 - beta_one) * grad
        new_second = beta_two * second_ref[at] + (1.0 - beta_two) * grad * grad
        new_first_ref[at] = new_first
        new_second_ref[at] = new_second
        update_ref[at] = new_first / correct_one / (jnp.sqrt(new_second / correct_two) + epsilon)


def adam(scale, first_old, second_old, pieces):
    return kernel_call(
        functools.partial(adam_kernel, scale),
        [VMEM] * 10,
        [struct((256, 256), F32)] * 3 + [struct((64, 128), F32)],
        5,
        (1 << 20, 2 << 20),
        [first_old, second_old, *pieces],
    )


def shards(proj_in, kv_grad, normed, norm_grad, first_moment, second_moment):
    return update_of(proj_in[0], kv_grad[0], normed, norm_grad, first_moment[0], second_moment[0])


def update_of(inputs, rows, normed, norm_grad, first_moment, second_moment):
    replicas = lax.axis_size(DP)
    gain = jnp.sum(norm_grad.astype(F32) * normed.astype(F32), axis=1).reshape(64, 128)
    starts = [ordered(0, rows, [gain]), ordered(1, rows, [])]

    def gathered(k):
        own = {0: starts[k]}
        up = down = starts[k]
        for step in (1, 2, 3, 4):
            if step < 4 or k == 0:
                up = shift(up, 1)
                own[4 if step == 4 else -step] = up
            if step < 4 or k == 1:
                down = shift(down, -1)
                own[step] = down
        blocks = []
        for step in STEPS:
            blocks += [own[step], swap(own[step], "c", 1)]
        return blocks

    gathers = [gathered(k) for k in range(2)]
    mine = turned(inputs, 0)
    other = swap(turned(inputs, 1), "yh", 1)

    in_x, in_y = [], []
    for k in range(2):
        outs = product(k, mine, other, gathers[k])
        by_x, by_y = outs[:4], outs[4:]
        in_x += [by_x[0]] + [swap(by_x[j], "x", j) for j in (1, 2, 3)]
        in_y += [by_y[0]] + [along_y(by_y[ab], ab) for ab in (1, 2, 3)]
    by_y = cut_sum(sum_rows_kernel, in_x, 160)
    by_x = cut_sum(sum_columns_kernel, in_y, 128)
    pieces = [by_y[0]] + [along_y(by_y[ab], ab) for ab in (1, 2, 3)]
    pieces += [by_x[0]] + [swap(by_x[j], "x", j) for j in (1, 2, 3)]
    new_first, new_second, update, gain = adam(1.0 / replicas, first_moment, second_moment, pieces)
    return (new_first[None], new_second[None], update[None], gain.reshape(1, 8192))


def solution(mesh):
    finer = Mesh(mesh.devices.reshape(4, 2, 2, 8, 2), AXES)
    return jax.shard_map(
        shards,
        mesh=finer,
        in_specs=(
            P(None, DP, TP),
            P(None, DP_TP, None),
            P(None, DP_TP, None),
            P(None, DP_TP, None),
            P(None, TP, DP),
            P(None, TP, DP),
        ),
        out_specs=(P(None, TP, DP), P(None, TP, DP), P(None, TP, DP), P()),
        check_vma=False,
    )
```

```python
import functools

import jax
import jax.numpy as jnp
from jax import lax
from jax.experimental import pallas as pl
from jax.experimental.pallas import tpu as pltpu
from jax.sharding import Mesh
from jax.sharding import PartitionSpec as P

AXES = ("x", "yl", "yh", "z", "c")
DP = ("x", "yl")
TP = ("yh", "z", "c")
DP_TP = AXES

beta_one = 0.9
beta_two = 0.95
correct_one = 0.19
correct_two = 0.0975
epsilon = 1e-08

F32 = jnp.float32
BF16 = jnp.bfloat16
VMEM = pl.BlockSpec(memory_space=pltpu.VMEM)
BY_X, BY_Y = 112, 144
STEPS = (0, -1, 1, -2, 2, -3, 3, 4)


def struct(shape, dtype):
    return jax.ShapeDtypeStruct(shape, dtype)


def cost(flops, bytes_moved):
    return pl.CostEstimate(flops=flops, bytes_accessed=bytes_moved, transcendentals=0)


def swap(array, axis, mask):
    size = lax.axis_size(axis)
    return lax.ppermute(array, axis, [(i, i ^ mask) for i in range(size)])


def shift(array, step):
    size = lax.axis_size("z")
    return lax.ppermute(array, "z", [(i, (i + step) % size) for i in range(size)])


def along_y(array, ab):
    if ab == 1:
        return swap(array, "yl", 1)
    if ab == 2:
        return swap(array, "yh", 1)
    return swap(array, ("yl", "yh"), 3)


def kernel_call(kernel, in_specs, out_shape, limit, estimate, operands, scratch=()):
    return pl.pallas_call(
        kernel,
        in_specs=in_specs,
        out_specs=[VMEM] * len(out_shape),
        out_shape=out_shape,
        scratch_shapes=list(scratch),
        cost_estimate=cost(*estimate),
        compiler_params=pltpu.CompilerParams(vmem_limit_bytes=limit << 20),
    )(*operands)


def order_kernel(k, rows_ref, *refs):
    out = refs[-1]
    x, yl = lax.axis_index("x"), lax.axis_index("yl")
    for j in range(4):
        for b in range(2):
            owner = (x ^ j) * 2 + (yl ^ b)
            to = (j * 2 + b) * 128
            start = pl.multiple_of(owner * 256 + k * 128, 128)
            out[:128, to : to + 128] = rows_ref[:, pl.ds(start, 128)]
    if k == 0:
        for q in range(8):
            sums = refs[0][q * 8 : (q + 1) * 8, :]
            high = sums.astype(BF16).astype(F32)
            out[128:144, q * 128 : (q + 1) * 128] = jnp.concatenate([high, sums - high]).astype(BF16)


def ordered(k, rows, gain):
    out = struct((144 if k == 0 else 128, 1024), BF16)
    specs = [VMEM] * (1 + len(gain))
    return kernel_call(
        functools.partial(order_kernel, k), specs, [out], 4, (1 << 20, 1 << 20), [rows, *gain]
    )[0]


def turn_kernel(away, inputs_ref, out_ref):
    half, z, c = lax.axis_index("yh") ^ away, lax.axis_index("z"), lax.axis_index("c")
    for p, step in enumerate(STEPS):
        for own in range(2):
            start = half * 2048 + ((z + step + 8) % 8) * 256 + (c ^ own) * 128
            block = inputs_ref[pl.ds(pl.multiple_of(start, 128), 128), :]
            to = (p * 2 + own) * 128
            out_ref[:, to : to + 128] = block.T


def turned(inputs, away):
    return kernel_call(
        functools.partial(turn_kernel, away),
        [VMEM],
        [struct((256, 2048), BF16)],
        6,
        (1 << 22, 2 << 20),
        [inputs],
    )[0]


def part_kernel(k, mine_ref, other_ref, *refs):
    blocks, outs, refs = refs[:14], refs[14:22], refs[22:]
    if k == 0:
        gains_ref, refs = refs[0], refs[1:]
        for i, block in enumerate(blocks):
            gains_ref[source_of(i)] = block[128:144, :]
    rows, result = refs

    @pl.loop(0, 4)
    def _(j):
        columns = pl.ds(pl.multiple_of(j * 256, 256), 256)
        for i, block in enumerate(blocks):
            rows[i * 128 : (i + 1) * 128, :] = block[:128, columns]
        right = rows[...]
        result[:256, :] = jnp.dot(mine_ref[:, :1792], right, preferred_element_type=F32)
        result[256:, :] = jnp.dot(other_ref[:, :1792], right, preferred_element_type=F32)
        for at in range(4):

            @pl.when(j == at)
            def _():
                outs[at][:BY_X, :] = result[:BY_X, :]
                outs[at][BY_X : 2 * BY_X, :] = result[256 : 256 + BY_X, :]

        to = pl.multiple_of(j * 128, 128)
        for a in range(2):
            for b in range(2):
                outs[4 + a * 2 + b][:, pl.ds(to, 128)] = result[
                    a * 256 + BY_X : a * 256 + 256, b * 128 : (b + 1) * 128
                ]


def source_of(i):
    z, c = lax.axis_index("z"), lax.axis_index("c")
    return ((z + STEPS[i // 2] + 8) % 8) * 2 + (c ^ (i % 2))


def product_kernel(k, mine_ref, other_ref, own_ref, swapped_ref, *refs):
    parts, refs = refs[:8], refs[8:]
    if k == 0:
        gains_ref, refs = refs[0], refs[1:]
    outs = refs
    for j in range(4):
        columns = slice(j * 256, (j + 1) * 256)
        right = jnp.concatenate([own_ref[:128, columns], swapped_ref[:128, columns]], axis=0)
        for a, left in enumerate((mine_ref, other_ref)):
            result = jnp.dot(left[:, 1792:], right, preferred_element_type=F32)
            at = slice(a * BY_X, (a + 1) * BY_X)
            outs[j][at, :] = parts[j][at, :] + result[:BY_X]
            for b in range(2):
                to = slice(j * 128, (j + 1) * 128)
                piece = 4 + a * 2 + b
                outs[piece][:, to] = parts[piece][:, to] + result[BY_X:, b * 128 : (b + 1) * 128]
    if k == 0:
        late = [(source_of(14), own_ref[128:144, :].astype(F32)), (source_of(15), swapped_ref[128:144, :].astype(F32))]
        total = jnp.zeros((16, 1024), F32)
        for i in range(16):
            value = gains_ref[i].astype(F32)
            for source, here in late:
                value = jnp.where(source == i, here, value)
            total = total + value
        total = total[:8] + total[8:]
        for q in range(8):
            at = slice(2 * BY_X + (q % 4) * 8, 2 * BY_X + (q % 4) * 8 + 8)
            to = slice((q // 4) * 128, (q // 4) * 128 + 128)
            for j in range(4):
                outs[j][at, to] = total[:, q * 128 : (q + 1) * 128]


def product(k, mine, other, blocks):
    pieces = [struct((BY_Y, 512), F32)] * 4
    scratch = [pltpu.VMEM((1792, 256), BF16), pltpu.VMEM((512, 256), F32)]
    gains = [struct((16, 16, 1024), BF16)] if k == 0 else []
    parts = kernel_call(
        functools.partial(part_kernel, k),
        [VMEM] * 16,
        [struct((2 * BY_X, 256), F32)] * 4 + pieces + gains,
        14,
        (2 * 512 * 1792 * 1024, 8 << 20),
        [mine, other, *blocks[:14]],
        scratch,
    )
    return kernel_call(
        functools.partial(product_kernel, k),
        [VMEM] * (4 + len(parts)),
        [struct((2 * BY_X + (32 if k == 0 else 0), 256), F32)] * 4 + pieces,
        14,
        (2 * 512 * 256 * 1024, 4 << 20),
        [mine, other, *blocks[14:], *parts],
    )


def sum_of(refs, at=slice(None)):
    own, one, two, three = (ref[at, :] for ref in refs)
    return (own + one) + (two + three)


def sum_rows_kernel(*refs):
    outs = refs[8:]
    for k in range(2):
        total = sum_of(refs[k * 4 : k * 4 + 4])
        for a in range(2):
            for b in range(2):
                outs[a * 2 + b][:BY_X, k * 128 : (k + 1) * 128] = total[
                    a * BY_X : (a + 1) * BY_X, b * 128 : (b + 1) * 128
                ]
        if k == 0:
            for out in outs:
                out[BY_X : BY_X + 32, :] = total[2 * BY_X : 2 * BY_X + 32, :]


def sum_columns_kernel(*refs):
    outs = refs[8:]
    for k in range(2):
        total = sum_of(refs[k * 4 : k * 4 + 4])
        for j in range(4):
            outs[j][:, k * 128 : (k + 1) * 128] = total[:, j * 128 : (j + 1) * 128]


def cut_sum(kernel, parts, rows):
    return kernel_call(
        kernel, [VMEM] * 8, [struct((rows, 256), F32)] * 4, 5, (1 << 18, 1 << 20), parts
    )


def adam_kernel(scale, first_ref, second_ref, *refs):
    pieces, (new_first_ref, new_second_ref, update_ref, gain_ref) = refs[:8], refs[8:]
    gain = sum_of(pieces[:4], slice(BY_X, BY_X + 32)) * scale
    gain_ref[:32, :] = gain[:, :128]
    gain_ref[32:, :] = gain[:, 128:]
    for four, start, rows in ((pieces[:4], 0, BY_X), (pieces[4:], BY_X, BY_Y)):
        grad = sum_of(four, slice(0, rows)) * scale
        at = (slice(start, start + rows), slice(None))
        new_first = beta_one * first_ref[at] + (1.0 - beta_one) * grad
        new_second = beta_two * second_ref[at] + (1.0 - beta_two) * grad * grad
        new_first_ref[at] = new_first
        new_second_ref[at] = new_second
        update_ref[at] = new_first / correct_one / (jnp.sqrt(new_second / correct_two) + epsilon)


def adam(scale, first_old, second_old, pieces):
    return kernel_call(
        functools.partial(adam_kernel, scale),
        [VMEM] * 10,
        [struct((256, 256), F32)] * 3 + [struct((64, 128), F32)],
        5,
        (1 << 20, 2 << 20),
        [first_old, second_old, *pieces],
    )


def shards(proj_in, kv_grad, normed, norm_grad, first_moment, second_moment):
    return update_of(proj_in[0], kv_grad[0], normed, norm_grad, first_moment[0], second_moment[0])


def update_of(inputs, rows, normed, norm_grad, first_moment, second_moment):
    replicas = lax.axis_size(DP)
    gain = jnp.sum(norm_grad.astype(F32) * normed.astype(F32), axis=1).reshape(64, 128)
    starts = [ordered(0, rows, [gain]), ordered(1, rows, [])]

    def gathered(k):
        own = {0: starts[k]}
        up = down = starts[k]
        for step in (1, 2, 3, 4):
            if step < 4 or k == 0:
                up = shift(up, 1)
                own[4 if step == 4 else -step] = up
            if step < 4 or k == 1:
                down = shift(down, -1)
                own[step] = down
        blocks = []
        for step in STEPS:
            blocks += [own[step], swap(own[step], "c", 1)]
        return blocks

    gathers = [gathered(k) for k in range(2)]
    mine = turned(inputs, 0)
    other = swap(turned(inputs, 1), "yh", 1)

    in_x, in_y = [], []
    for k in range(2):
        outs = product(k, mine, other, gathers[k])
        by_x, by_y = outs[:4], outs[4:]
        in_x += [by_x[0]] + [swap(by_x[j], "x", j) for j in (1, 2, 3)]
        in_y += [by_y[0]] + [along_y(by_y[ab], ab) for ab in (1, 2, 3)]
    by_y = cut_sum(sum_rows_kernel, in_x, BY_X + 32)
    by_x = cut_sum(sum_columns_kernel, in_y, BY_Y)
    pieces = [by_y[0]] + [along_y(by_y[ab], ab) for ab in (1, 2, 3)]
    pieces += [by_x[0]] + [swap(by_x[j], "x", j) for j in (1, 2, 3)]
    new_first, new_second, update, gain = adam(1.0 / replicas, first_moment, second_moment, pieces)
    return (new_first[None], new_second[None], update[None], gain.reshape(1, 8192))


def solution(mesh):
    finer = Mesh(mesh.devices.reshape(4, 2, 2, 8, 2), AXES)
    return jax.shard_map(
        shards,
        mesh=finer,
        in_specs=(
            P(None, DP, TP),
            P(None, DP_TP, None),
            P(None, DP_TP, None),
            P(None, DP_TP, None),
            P(None, TP, DP),
            P(None, TP, DP),
        ),
        out_specs=(P(None, TP, DP), P(None, TP, DP), P(None, TP, DP), P()),
        check_vma=False,
    )
```

```python
import functools

import jax
import jax.numpy as jnp
from jax import lax
from jax.experimental import pallas as pl
from jax.experimental.pallas import tpu as pltpu
from jax.sharding import Mesh
from jax.sharding import PartitionSpec as P

AXES = ("x", "yl", "yh", "z", "c")
DP = ("x", "yl")
TP = ("yh", "z", "c")
DP_TP = AXES

beta_one = 0.9
beta_two = 0.95
correct_one = 0.19
correct_two = 0.0975
epsilon = 1e-08

F32 = jnp.float32
BF16 = jnp.bfloat16
VMEM = pl.BlockSpec(memory_space=pltpu.VMEM)
BY_X, BY_Y = 112, 144
STEPS = (0, -1, 1, -2, 2, -3, 3, 4)


def struct(shape, dtype):
    return jax.ShapeDtypeStruct(shape, dtype)


def cost(flops, bytes_moved):
    return pl.CostEstimate(flops=flops, bytes_accessed=bytes_moved, transcendentals=0)


def swap(array, axis, mask):
    size = lax.axis_size(axis)
    return lax.ppermute(array, axis, [(i, i ^ mask) for i in range(size)])


def shift(array, step):
    size = lax.axis_size("z")
    return lax.ppermute(array, "z", [(i, (i + step) % size) for i in range(size)])


def along_y(array, ab):
    if ab == 1:
        return swap(array, "yl", 1)
    if ab == 2:
        return swap(array, "yh", 1)
    return swap(array, ("yl", "yh"), 3)


def kernel_call(kernel, in_specs, out_shape, limit, estimate, operands, scratch=()):
    return pl.pallas_call(
        kernel,
        in_specs=in_specs,
        out_specs=[VMEM] * len(out_shape),
        out_shape=out_shape,
        scratch_shapes=list(scratch),
        cost_estimate=cost(*estimate),
        compiler_params=pltpu.CompilerParams(vmem_limit_bytes=limit << 20),
    )(*operands)


def order_kernel(k, rows_ref, *refs):
    out = refs[-1]
    x, yl = lax.axis_index("x"), lax.axis_index("yl")
    for j in range(4):
        for b in range(2):
            owner = (x ^ j) * 2 + (yl ^ b)
            to = (j * 2 + b) * 128
            start = pl.multiple_of(owner * 256 + k * 128, 128)
            out[:128, to : to + 128] = rows_ref[:, pl.ds(start, 128)]
    if k == 0:
        for q in range(8):
            sums = refs[0][q * 8 : (q + 1) * 8, :]
            high = sums.astype(BF16).astype(F32)
            out[128:144, q * 128 : (q + 1) * 128] = jnp.concatenate([high, sums - high]).astype(BF16)


def ordered(k, rows, gain):
    out = struct((144 if k == 0 else 128, 1024), BF16)
    specs = [VMEM] * (1 + len(gain))
    return kernel_call(
        functools.partial(order_kernel, k), specs, [out], 4, (1 << 20, 1 << 20), [rows, *gain]
    )[0]


def turn_kernel(away, inputs_ref, out_ref):
    half, z, c = lax.axis_index("yh") ^ away, lax.axis_index("z"), lax.axis_index("c")
    for p, step in enumerate(STEPS):
        for own in range(2):
            start = half * 2048 + ((z + step + 8) % 8) * 256 + (c ^ own) * 128
            block = inputs_ref[pl.ds(pl.multiple_of(start, 128), 128), :]
            to = (p * 2 + own) * 128
            out_ref[:, to : to + 128] = block.T


def turned(inputs, away):
    return kernel_call(
        functools.partial(turn_kernel, away),
        [VMEM],
        [struct((256, 2048), BF16)],
        6,
        (1 << 22, 2 << 20),
        [inputs],
    )[0]


def part_kernel(k, mine_ref, other_ref, *refs):
    blocks, outs, refs = refs[:14], refs[14:22], refs[22:]
    if k == 0:
        gains_ref, refs = refs[0], refs[1:]
        for i, block in enumerate(blocks):
            gains_ref[source_of(i)] = block[128:144, :]
    rows, result = refs

    @pl.loop(0, 4)
    def _(j):
        columns = pl.ds(pl.multiple_of(j * 256, 256), 256)
        for i, block in enumerate(blocks):
            rows[i * 128 : (i + 1) * 128, :] = block[:128, columns]
        right = rows[...]
        result[:256, :] = jnp.dot(mine_ref[:, :1792], right, preferred_element_type=F32)
        result[256:, :] = jnp.dot(other_ref[:, :1792], right, preferred_element_type=F32)
        for at in range(4):

            @pl.when(j == at)
            def _():
                outs[at][:BY_X, :] = result[:BY_X, :]
                outs[at][BY_X : 2 * BY_X, :] = result[256 : 256 + BY_X, :]

        to = pl.multiple_of(j * 128, 128)
        for a in range(2):
            for b in range(2):
                outs[4 + a * 2 + b][:, pl.ds(to, 128)] = result[
                    a * 256 + BY_X : a * 256 + 256, b * 128 : (b + 1) * 128
                ]


def source_of(i):
    z, c = lax.axis_index("z"), lax.axis_index("c")
    return ((z + STEPS[i // 2] + 8) % 8) * 2 + (c ^ (i % 2))


def product_kernel(k, mine_ref, other_ref, own_ref, swapped_ref, *refs):
    parts, refs = refs[:8], refs[8:]
    if k == 0:
        gains_ref, refs = refs[0], refs[1:]
    outs = refs
    for j in range(4):
        columns = slice(j * 256, (j + 1) * 256)
        right = jnp.concatenate([own_ref[:128, columns], swapped_ref[:128, columns]], axis=0)
        for a, left in enumerate((mine_ref, other_ref)):
            result = jnp.dot(left[:, 1792:], right, preferred_element_type=F32)
            at = slice(a * BY_X, (a + 1) * BY_X)
            outs[j][at, :] = parts[j][at, :] + result[:BY_X]
            for b in range(2):
                to = slice(j * 128, (j + 1) * 128)
                piece = 4 + a * 2 + b
                outs[piece][:, to] = parts[piece][:, to] + result[BY_X:, b * 128 : (b + 1) * 128]
    if k == 0:
        late = [(source_of(14), own_ref[128:144, :].astype(F32)), (source_of(15), swapped_ref[128:144, :].astype(F32))]
        total = jnp.zeros((16, 1024), F32)
        for i in range(16):
            value = gains_ref[i].astype(F32)
            for source, here in late:
                value = jnp.where(source == i, here, value)
            total = total + value
        total = total[:8] + total[8:]
        for q in range(8):
            at = slice(2 * BY_X + (q % 4) * 8, 2 * BY_X + (q % 4) * 8 + 8)
            to = slice((q // 4) * 128, (q // 4) * 128 + 128)
            for j in range(4):
                outs[j][at, to] = total[:, q * 128 : (q + 1) * 128]


def product(k, mine, other, blocks):
    pieces = [struct((BY_Y, 512), F32)] * 4
    scratch = [pltpu.VMEM((1792, 256), BF16), pltpu.VMEM((512, 256), F32)]
    gains = [struct((16, 16, 1024), BF16)] if k == 0 else []
    parts = kernel_call(
        functools.partial(part_kernel, k),
        [VMEM] * 16,
        [struct((2 * BY_X, 256), F32)] * 4 + pieces + gains,
        14,
        (2 * 512 * 1792 * 1024, 8 << 20),
        [mine, other, *blocks[:14]],
        scratch,
    )
    return kernel_call(
        functools.partial(product_kernel, k),
        [VMEM] * (4 + len(parts)),
        [struct((2 * BY_X + (32 if k == 0 else 0), 256), F32)] * 4 + pieces,
        14,
        (2 * 512 * 256 * 1024, 4 << 20),
        [mine, other, *blocks[14:], *parts],
    )


def sum_of(refs, at=slice(None)):
    own, one, two, three = (ref[at, :] for ref in refs)
    return (own + one) + (two + three)


def sum_rows_kernel(*refs):
    outs = refs[8:]
    for k in range(2):
        total = sum_of(refs[k * 4 : k * 4 + 4])
        for a in range(2):
            for b in range(2):
                outs[a * 2 + b][:BY_X, k * 128 : (k + 1) * 128] = total[
                    a * BY_X : (a + 1) * BY_X, b * 128 : (b + 1) * 128
                ]
        if k == 0:
            for out in outs:
                out[BY_X : BY_X + 32, :] = total[2 * BY_X : 2 * BY_X + 32, :]


def sum_columns_kernel(*refs):
    total = sum_of(refs[:4])
    for j in range(4):
        refs[4 + j][...] = total[:, j * 128 : (j + 1) * 128]


def cut_sum(kernel, parts, shape):
    return kernel_call(
        kernel, [VMEM] * len(parts), [struct(shape, F32)] * 4, 5, (1 << 18, 1 << 20), parts
    )


def adam_kernel(scale, first_ref, second_ref, *refs):
    pieces, (new_first_ref, new_second_ref, update_ref, gain_ref) = refs[:12], refs[12:]
    gain = sum_of(pieces[:4], slice(BY_X, BY_X + 32)) * scale
    gain_ref[:32, :] = gain[:, :128]
    gain_ref[32:, :] = gain[:, 128:]
    for four, start, rows, columns in (
        (pieces[:4], 0, BY_X, slice(None)),
        (pieces[4:8], BY_X, BY_Y, slice(0, 128)),
        (pieces[8:], BY_X, BY_Y, slice(128, 256)),
    ):
        grad = sum_of(four, slice(0, rows)) * scale
        at = (slice(start, start + rows), columns)
        new_first = beta_one * first_ref[at] + (1.0 - beta_one) * grad
        new_second = beta_two * second_ref[at] + (1.0 - beta_two) * grad * grad
        new_first_ref[at] = new_first
        new_second_ref[at] = new_second
        update_ref[at] = new_first / correct_one / (jnp.sqrt(new_second / correct_two) + epsilon)


def adam(scale, first_old, second_old, pieces):
    return kernel_call(
        functools.partial(adam_kernel, scale),
        [VMEM] * 14,
        [struct((256, 256), F32)] * 3 + [struct((64, 128), F32)],
        5,
        (1 << 20, 2 << 20),
        [first_old, second_old, *pieces],
    )


def shards(proj_in, kv_grad, normed, norm_grad, first_moment, second_moment):
    return update_of(proj_in[0], kv_grad[0], normed, norm_grad, first_moment[0], second_moment[0])


def update_of(inputs, rows, normed, norm_grad, first_moment, second_moment):
    replicas = lax.axis_size(DP)
    gain = jnp.sum(norm_grad.astype(F32) * normed.astype(F32), axis=1).reshape(64, 128)
    starts = [ordered(0, rows, [gain]), ordered(1, rows, [])]

    def gathered(k):
        own = {0: starts[k]}
        up = down = starts[k]
        for step in (1, 2, 3, 4):
            if step < 4 or k == 0:
                up = shift(up, 1)
                own[4 if step == 4 else -step] = up
            if step < 4 or k == 1:
                down = shift(down, -1)
                own[step] = down
        blocks = []
        for step in STEPS:
            blocks += [own[step], swap(own[step], "c", 1)]
        return blocks

    gathers = [gathered(k) for k in range(2)]
    mine = turned(inputs, 0)
    other = swap(turned(inputs, 1), "yh", 1)

    in_x, in_y = [], []
    for k in range(2):
        outs = product(k, mine, other, gathers[k])
        by_x, by_y = outs[:4], outs[4:]
        in_x += [by_x[0]] + [swap(by_x[j], "x", j) for j in (1, 2, 3)]
        in_y += [by_y[0]] + [along_y(by_y[ab], ab) for ab in (1, 2, 3)]
    by_y = cut_sum(sum_rows_kernel, in_x, (BY_X + 32, 256))
    pieces = [by_y[0]] + [along_y(by_y[ab], ab) for ab in (1, 2, 3)]
    for k in range(2):
        by_x = cut_sum(sum_columns_kernel, in_y[k * 4 : k * 4 + 4], (BY_Y, 128))
        pieces += [by_x[0]] + [swap(by_x[j], "x", j) for j in (1, 2, 3)]
    new_first, new_second, update, gain = adam(1.0 / replicas, first_moment, second_moment, pieces)
    return (new_first[None], new_second[None], update[None], gain.reshape(1, 8192))


def solution(mesh):
    finer = Mesh(mesh.devices.reshape(4, 2, 2, 8, 2), AXES)
    return jax.shard_map(
        shards,
        mesh=finer,
        in_specs=(
            P(None, DP, TP),
            P(None, DP_TP, None),
            P(None, DP_TP, None),
            P(None, DP_TP, None),
            P(None, TP, DP),
            P(None, TP, DP),
        ),
        out_specs=(P(None, TP, DP), P(None, TP, DP), P(None, TP, DP), P()),
        check_vma=False,
    )
```

```python
import functools

import jax
import jax.numpy as jnp
from jax import lax
from jax.experimental import pallas as pl
from jax.experimental.pallas import tpu as pltpu
from jax.sharding import Mesh
from jax.sharding import PartitionSpec as P

AXES = ("x", "yl", "yh", "z", "c")
DP = ("x", "yl")
TP = ("yh", "z", "c")
DP_TP = AXES

beta_one = 0.9
beta_two = 0.95
correct_one = 0.19
correct_two = 0.0975
epsilon = 1e-08

F32 = jnp.float32
BF16 = jnp.bfloat16
VMEM = pl.BlockSpec(memory_space=pltpu.VMEM)
BY_X, BY_Y = 112, 144
STEPS = (0, -1, 1, -2, 2, -3, 3, 4)


def struct(shape, dtype):
    return jax.ShapeDtypeStruct(shape, dtype)


def cost(flops, bytes_moved):
    return pl.CostEstimate(flops=flops, bytes_accessed=bytes_moved, transcendentals=0)


def swap(array, axis, mask):
    size = lax.axis_size(axis)
    return lax.ppermute(array, axis, [(i, i ^ mask) for i in range(size)])


def shift(array, step):
    size = lax.axis_size("z")
    return lax.ppermute(array, "z", [(i, (i + step) % size) for i in range(size)])


def along_y(array, ab):
    if ab == 1:
        return swap(array, "yl", 1)
    if ab == 2:
        return swap(array, "yh", 1)
    return swap(array, ("yl", "yh"), 3)


def kernel_call(kernel, in_specs, out_shape, limit, estimate, operands, scratch=()):
    return pl.pallas_call(
        kernel,
        in_specs=in_specs,
        out_specs=[VMEM] * len(out_shape),
        out_shape=out_shape,
        scratch_shapes=list(scratch),
        cost_estimate=cost(*estimate),
        compiler_params=pltpu.CompilerParams(vmem_limit_bytes=limit << 20),
    )(*operands)


def order_kernel(k, rows_ref, *refs):
    out = refs[-1]
    x, yl = lax.axis_index("x"), lax.axis_index("yl")
    for j in range(4):
        for b in range(2):
            owner = (x ^ j) * 2 + (yl ^ b)
            to = (j * 2 + b) * 128
            start = pl.multiple_of(owner * 256 + k * 128, 128)
            out[:128, to : to + 128] = rows_ref[:, pl.ds(start, 128)]
    if k == 0:
        for q in range(8):
            sums = refs[0][q * 8 : (q + 1) * 8, :]
            high = sums.astype(BF16).astype(F32)
            out[128:144, q * 128 : (q + 1) * 128] = jnp.concatenate([high, sums - high]).astype(BF16)


def ordered(k, rows, gain):
    out = struct((144 if k == 0 else 128, 1024), BF16)
    specs = [VMEM] * (1 + len(gain))
    return kernel_call(
        functools.partial(order_kernel, k), specs, [out], 4, (1 << 20, 1 << 20), [rows, *gain]
    )[0]


def turn_kernel(away, inputs_ref, out_ref):
    half, z, c = lax.axis_index("yh") ^ away, lax.axis_index("z"), lax.axis_index("c")
    for p, step in enumerate(STEPS):
        for own in range(2):
            start = half * 2048 + ((z + step + 8) % 8) * 256 + (c ^ own) * 128
            block = inputs_ref[pl.ds(pl.multiple_of(start, 128), 128), :]
            to = (p * 2 + own) * 128
            out_ref[:, to : to + 128] = block.T


def turned(inputs, away):
    return kernel_call(
        functools.partial(turn_kernel, away),
        [VMEM],
        [struct((256, 2048), BF16)],
        6,
        (1 << 22, 2 << 20),
        [inputs],
    )[0]


def part_kernel(k, mine_ref, other_ref, *refs):
    blocks, outs, refs = refs[:14], refs[14:22], refs[22:]
    if k == 0:
        gains_ref, refs = refs[0], refs[1:]
        for i, block in enumerate(blocks):
            gains_ref[source_of(i)] = block[128:144, :]
    rows, result = refs

    @pl.loop(0, 4)
    def _(j):
        columns = pl.ds(pl.multiple_of(j * 256, 256), 256)
        for i, block in enumerate(blocks):
            rows[i * 128 : (i + 1) * 128, :] = block[:128, columns]
        right = rows[...]
        result[:256, :] = jnp.dot(mine_ref[:, :1792], right, preferred_element_type=F32)
        result[256:, :] = jnp.dot(other_ref[:, :1792], right, preferred_element_type=F32)
        for at in range(4):

            @pl.when(j == at)
            def _():
                outs[at][:BY_X, :] = result[:BY_X, :]
                outs[at][BY_X : 2 * BY_X, :] = result[256 : 256 + BY_X, :]

        to = pl.multiple_of(j * 128, 128)
        for a in range(2):
            for b in range(2):
                outs[4 + a * 2 + b][:, pl.ds(to, 128)] = result[
                    a * 256 + BY_X : a * 256 + 256, b * 128 : (b + 1) * 128
                ]


def source_of(i):
    z, c = lax.axis_index("z"), lax.axis_index("c")
    return ((z + STEPS[i // 2] + 8) % 8) * 2 + (c ^ (i % 2))


def product_kernel(k, mine_ref, other_ref, *refs):
    late, parts, refs = refs[: 2 + 2 * k], refs[2 + 2 * k : 10 + 2 * k], refs[10 + 2 * k :]
    if k == 0:
        gains_ref, refs = refs[0], refs[1:]
    outs = refs
    for j in range(4):
        columns = slice(j * 256, (j + 1) * 256)
        right = jnp.concatenate([ref[: 128 // (1 + k), columns] for ref in late], axis=0)
        for a, left in enumerate((mine_ref, other_ref)):
            result = jnp.dot(left[:, 1792:], right, preferred_element_type=F32)
            at = slice(a * BY_X, (a + 1) * BY_X)
            outs[j][at, :] = parts[j][at, :] + result[:BY_X]
            for b in range(2):
                to = slice(j * 128, (j + 1) * 128)
                piece = 4 + a * 2 + b
                outs[piece][:, to] = parts[piece][:, to] + result[BY_X:, b * 128 : (b + 1) * 128]
    if k == 0:
        late = [(source_of(14 + i), ref[128:144, :].astype(F32)) for i, ref in enumerate(late)]
        total = jnp.zeros((16, 1024), F32)
        for i in range(16):
            value = gains_ref[i].astype(F32)
            for source, here in late:
                value = jnp.where(source == i, here, value)
            total = total + value
        total = total[:8] + total[8:]
        for q in range(8):
            at = slice(2 * BY_X + (q % 4) * 8, 2 * BY_X + (q % 4) * 8 + 8)
            to = slice((q // 4) * 128, (q // 4) * 128 + 128)
            for j in range(4):
                outs[j][at, to] = total[:, q * 128 : (q + 1) * 128]


def product(k, mine, other, blocks, last):
    pieces = [struct((BY_Y, 512), F32)] * 4
    scratch = [pltpu.VMEM((1792, 256), BF16), pltpu.VMEM((512, 256), F32)]
    gains = [struct((16, 16, 1024), BF16)] if k == 0 else []
    parts = kernel_call(
        functools.partial(part_kernel, k),
        [VMEM] * 16,
        [struct((2 * BY_X, 256), F32)] * 4 + pieces + gains,
        14,
        (2 * 512 * 1792 * 1024, 8 << 20),
        [mine, other, *blocks],
        scratch,
    )
    return kernel_call(
        functools.partial(product_kernel, k),
        [VMEM] * (2 + len(last) + len(parts)),
        [struct((2 * BY_X + (32 if k == 0 else 0), 256), F32)] * 4 + pieces,
        14,
        (2 * 512 * 256 * 1024, 4 << 20),
        [mine, other, *last, *parts],
    )


def sum_of(refs, at=slice(None)):
    own, one, two, three = (ref[at, :] for ref in refs)
    return (own + one) + (two + three)


def sum_rows_kernel(*refs):
    outs = refs[8:]
    for k in range(2):
        total = sum_of(refs[k * 4 : k * 4 + 4])
        for a in range(2):
            for b in range(2):
                outs[a * 2 + b][:BY_X, k * 128 : (k + 1) * 128] = total[
                    a * BY_X : (a + 1) * BY_X, b * 128 : (b + 1) * 128
                ]
        if k == 0:
            for out in outs:
                out[BY_X : BY_X + 32, :] = total[2 * BY_X : 2 * BY_X + 32, :]


def sum_columns_kernel(*refs):
    outs = refs[8:]
    for k in range(2):
        total = sum_of(refs[k * 4 : k * 4 + 4])
        for j in range(4):
            outs[j][:, k * 128 : (k + 1) * 128] = total[:, j * 128 : (j + 1) * 128]


def cut_sum(kernel, parts, rows):
    return kernel_call(
        kernel, [VMEM] * 8, [struct((rows, 256), F32)] * 4, 5, (1 << 18, 1 << 20), parts
    )


def adam_kernel(scale, first_ref, second_ref, *refs):
    pieces, (new_first_ref, new_second_ref, update_ref, gain_ref) = refs[:8], refs[8:]
    gain = sum_of(pieces[:4], slice(BY_X, BY_X + 32)) * scale
    gain_ref[:32, :] = gain[:, :128]
    gain_ref[32:, :] = gain[:, 128:]
    for four, start, rows in ((pieces[:4], 0, BY_X), (pieces[4:], BY_X, BY_Y)):
        grad = sum_of(four, slice(0, rows)) * scale
        at = (slice(start, start + rows), slice(None))
        new_first = beta_one * first_ref[at] + (1.0 - beta_one) * grad
        new_second = beta_two * second_ref[at] + (1.0 - beta_two) * grad * grad
        new_first_ref[at] = new_first
        new_second_ref[at] = new_second
        update_ref[at] = new_first / correct_one / (jnp.sqrt(new_second / correct_two) + epsilon)


def adam(scale, first_old, second_old, pieces):
    return kernel_call(
        functools.partial(adam_kernel, scale),
        [VMEM] * 10,
        [struct((256, 256), F32)] * 3 + [struct((64, 128), F32)],
        5,
        (1 << 20, 2 << 20),
        [first_old, second_old, *pieces],
    )


def shards(proj_in, kv_grad, normed, norm_grad, first_moment, second_moment):
    return update_of(proj_in[0], kv_grad[0], normed, norm_grad, first_moment[0], second_moment[0])


def update_of(inputs, rows, normed, norm_grad, first_moment, second_moment):
    replicas = lax.axis_size(DP)
    gain = jnp.sum(norm_grad.astype(F32) * normed.astype(F32), axis=1).reshape(64, 128)
    starts = [ordered(0, rows, [gain]), ordered(1, rows, [])]

    def gathered(k):
        own = {0: starts[k]}
        up = down = starts[k]
        for step in (1, 2, 3):
            up = shift(up, 1)
            down = shift(down, -1)
            own[-step], own[step] = up, down
        if k == 0:
            last = [shift(up, 1)]
        else:
            last = [shift(up[:64], 1), shift(down[64:], -1)]
        blocks = []
        for step in STEPS[:-1]:
            blocks += [own[step], swap(own[step], "c", 1)]
        return blocks, last + [swap(half, "c", 1) for half in last]

    gathers = [gathered(k) for k in range(2)]
    mine = turned(inputs, 0)
    other = swap(turned(inputs, 1), "yh", 1)

    in_x, in_y = [], []
    for k in range(2):
        outs = product(k, mine, other, *gathers[k])
        by_x, by_y = outs[:4], outs[4:]
        in_x += [by_x[0]] + [swap(by_x[j], "x", j) for j in (1, 2, 3)]
        in_y += [by_y[0]] + [along_y(by_y[ab], ab) for ab in (1, 2, 3)]
    by_y = cut_sum(sum_rows_kernel, in_x, BY_X + 32)
    by_x = cut_sum(sum_columns_kernel, in_y, BY_Y)
    pieces = [by_y[0]] + [along_y(by_y[ab], ab) for ab in (1, 2, 3)]
    pieces += [by_x[0]] + [swap(by_x[j], "x", j) for j in (1, 2, 3)]
    new_first, new_second, update, gain = adam(1.0 / replicas, first_moment, second_moment, pieces)
    return (new_first[None], new_second[None], update[None], gain.reshape(1, 8192))


def solution(mesh):
    finer = Mesh(mesh.devices.reshape(4, 2, 2, 8, 2), AXES)
    return jax.shard_map(
        shards,
        mesh=finer,
        in_specs=(
            P(None, DP, TP),
            P(None, DP_TP, None),
            P(None, DP_TP, None),
            P(None, DP_TP, None),
            P(None, TP, DP),
            P(None, TP, DP),
        ),
        out_specs=(P(None, TP, DP), P(None, TP, DP), P(None, TP, DP), P()),
        check_vma=False,
    )
```

```python
import functools

import jax
import jax.numpy as jnp
from jax import lax
from jax.experimental import pallas as pl
from jax.experimental.pallas import tpu as pltpu
from jax.sharding import Mesh
from jax.sharding import PartitionSpec as P

AXES = ("x", "yl", "yh", "z", "c")
DP = ("x", "yl")
TP = ("yh", "z", "c")
DP_TP = AXES

beta_one = 0.9
beta_two = 0.95
correct_one = 0.19
correct_two = 0.0975
epsilon = 1e-08

F32 = jnp.float32
BF16 = jnp.bfloat16
VMEM = pl.BlockSpec(memory_space=pltpu.VMEM)
BY_X, BY_Y = 112, 144
STEPS = (0, -1, 1, -2, 2, -3, 3, 4)


def struct(shape, dtype):
    return jax.ShapeDtypeStruct(shape, dtype)


def cost(flops, bytes_moved):
    return pl.CostEstimate(flops=flops, bytes_accessed=bytes_moved, transcendentals=0)


def swap(array, axis, mask):
    size = lax.axis_size(axis)
    return lax.ppermute(array, axis, [(i, i ^ mask) for i in range(size)])


def shift(array, step):
    size = lax.axis_size("z")
    return lax.ppermute(array, "z", [(i, (i + step) % size) for i in range(size)])


def along_y(array, ab):
    if ab == 1:
        return swap(array, "yl", 1)
    if ab == 2:
        return swap(array, "yh", 1)
    return swap(array, ("yl", "yh"), 3)


def kernel_call(kernel, in_specs, out_shape, limit, estimate, operands, scratch=()):
    return pl.pallas_call(
        kernel,
        in_specs=in_specs,
        out_specs=[VMEM] * len(out_shape),
        out_shape=out_shape,
        scratch_shapes=list(scratch),
        cost_estimate=cost(*estimate),
        compiler_params=pltpu.CompilerParams(vmem_limit_bytes=limit << 20),
    )(*operands)


def order_kernel(k, rows_ref, *refs):
    out = refs[-1]
    x, yl = lax.axis_index("x"), lax.axis_index("yl")
    for j in range(4):
        for b in range(2):
            owner = (x ^ j) * 2 + (yl ^ b)
            to = (j * 2 + b) * 128
            start = pl.multiple_of(owner * 256 + k * 128, 128)
            out[:128, to : to + 128] = rows_ref[:, pl.ds(start, 128)]
    if k == 0:
        for q in range(8):
            sums = refs[0][q * 8 : (q + 1) * 8, :]
            high = sums.astype(BF16).astype(F32)
            out[128:144, q * 128 : (q + 1) * 128] = jnp.concatenate([high, sums - high]).astype(BF16)


def ordered(k, rows, gain):
    out = struct((144 if k == 0 else 128, 1024), BF16)
    specs = [VMEM] * (1 + len(gain))
    return kernel_call(
        functools.partial(order_kernel, k), specs, [out], 4, (1 << 20, 1 << 20), [rows, *gain]
    )[0]


def turn_kernel(away, inputs_ref, out_ref):
    half, z, c = lax.axis_index("yh") ^ away, lax.axis_index("z"), lax.axis_index("c")
    for p, step in enumerate(STEPS):
        for own in range(2):
            start = half * 2048 + ((z + step + 8) % 8) * 256 + (c ^ own) * 128
            block = inputs_ref[pl.ds(pl.multiple_of(start, 128), 128), :]
            to = (p * 2 + own) * 128
            out_ref[:, to : to + 128] = block.T


def turned(inputs, away):
    return kernel_call(
        functools.partial(turn_kernel, away),
        [VMEM],
        [struct((256, 2048), BF16)],
        6,
        (1 << 22, 2 << 20),
        [inputs],
    )[0]


def part_kernel(k, mine_ref, other_ref, *refs):
    blocks, by_x_ref, by_y_ref, refs = refs[:14], refs[14], refs[15], refs[16:]
    if k == 0:
        gains_ref, refs = refs[0], refs[1:]
        for i, block in enumerate(blocks):
            gains_ref[source_of(i)] = block[128:144, :]
    rows = refs[0]

    @pl.loop(0, 4)
    def _(j):
        columns = pl.ds(pl.multiple_of(j * 256, 256), 256)
        for i, block in enumerate(blocks):
            rows[i * 128 : (i + 1) * 128, :] = block[:128, columns]
        right = rows[...]
        to = pl.ds(pl.multiple_of(j * 128, 128), 128)
        for a, left in enumerate((mine_ref, other_ref)):
            result = jnp.dot(left[:, :1792], right, preferred_element_type=F32)
            by_x_ref[j, a * BY_X : (a + 1) * BY_X, :] = result[:BY_X]
            for b in range(2):
                by_y_ref[a * 2 + b, :, to] = result[BY_X:, b * 128 : (b + 1) * 128]


def source_of(i):
    z, c = lax.axis_index("z"), lax.axis_index("c")
    return ((z + STEPS[i // 2] + 8) % 8) * 2 + (c ^ (i % 2))


def product_kernel(k, mine_ref, other_ref, own_ref, swapped_ref, *refs):
    by_x_ref, by_y_ref, refs = refs[0], refs[1], refs[2:]
    if k == 0:
        gains_ref, refs = refs[0], refs[1:]
    outs = refs
    for j in range(4):
        columns = slice(j * 256, (j + 1) * 256)
        right = jnp.concatenate([own_ref[:128, columns], swapped_ref[:128, columns]], axis=0)
        for a, left in enumerate((mine_ref, other_ref)):
            result = jnp.dot(left[:, 1792:], right, preferred_element_type=F32)
            at = slice(a * BY_X, (a + 1) * BY_X)
            outs[j][at, :] = by_x_ref[j, at, :] + result[:BY_X]
            for b in range(2):
                to = slice(j * 128, (j + 1) * 128)
                here = by_y_ref[a * 2 + b, :, to]
                outs[4 + a * 2 + b][:, to] = here + result[BY_X:, b * 128 : (b + 1) * 128]
    if k == 0:
        late = [(source_of(14), own_ref[128:144, :].astype(F32)), (source_of(15), swapped_ref[128:144, :].astype(F32))]
        total = jnp.zeros((16, 1024), F32)
        for i in range(16):
            value = gains_ref[i].astype(F32)
            for source, here in late:
                value = jnp.where(source == i, here, value)
            total = total + value
        total = total[:8] + total[8:]
        for q in range(8):
            at = slice(2 * BY_X + (q % 4) * 8, 2 * BY_X + (q % 4) * 8 + 8)
            to = slice((q // 4) * 128, (q // 4) * 128 + 128)
            for j in range(4):
                outs[j][at, to] = total[:, q * 128 : (q + 1) * 128]


def product(k, mine, other, blocks):
    pieces = [struct((BY_Y, 512), F32)] * 4
    gains = [struct((16, 16, 1024), BF16)] if k == 0 else []
    parts = kernel_call(
        functools.partial(part_kernel, k),
        [VMEM] * 16,
        [struct((4, 2 * BY_X, 256), F32), struct((4, BY_Y, 512), F32)] + gains,
        14,
        (2 * 512 * 1792 * 1024, 8 << 20),
        [mine, other, *blocks[:14]],
        [pltpu.VMEM((1792, 256), BF16)],
    )
    return kernel_call(
        functools.partial(product_kernel, k),
        [VMEM] * (4 + len(parts)),
        [struct((2 * BY_X + (32 if k == 0 else 0), 256), F32)] * 4 + pieces,
        14,
        (2 * 512 * 256 * 1024, 4 << 20),
        [mine, other, *blocks[14:], *parts],
    )


def sum_of(refs, at=slice(None)):
    own, one, two, three = (ref[at, :] for ref in refs)
    return (own + one) + (two + three)


def sum_rows_kernel(*refs):
    outs = refs[8:]
    for k in range(2):
        total = sum_of(refs[k * 4 : k * 4 + 4])
        for a in range(2):
            for b in range(2):
                outs[a * 2 + b][:BY_X, k * 128 : (k + 1) * 128] = total[
                    a * BY_X : (a + 1) * BY_X, b * 128 : (b + 1) * 128
                ]
        if k == 0:
            for out in outs:
                out[BY_X : BY_X + 32, :] = total[2 * BY_X : 2 * BY_X + 32, :]


def sum_columns_kernel(*refs):
    outs = refs[8:]
    for k in range(2):
        total = sum_of(refs[k * 4 : k * 4 + 4])
        for j in range(4):
            outs[j][:, k * 128 : (k + 1) * 128] = total[:, j * 128 : (j + 1) * 128]


def cut_sum(kernel, parts, rows):
    return kernel_call(
        kernel, [VMEM] * 8, [struct((rows, 256), F32)] * 4, 5, (1 << 18, 1 << 20), parts
    )


def adam_kernel(scale, first_ref, second_ref, *refs):
    pieces, (new_first_ref, new_second_ref, update_ref, gain_ref) = refs[:8], refs[8:]
    gain = sum_of(pieces[:4], slice(BY_X, BY_X + 32)) * scale
    gain_ref[:32, :] = gain[:, :128]
    gain_ref[32:, :] = gain[:, 128:]
    for four, start, rows in ((pieces[:4], 0, BY_X), (pieces[4:], BY_X, BY_Y)):
        grad = sum_of(four, slice(0, rows)) * scale
        at = (slice(start, start + rows), slice(None))
        new_first = beta_one * first_ref[at] + (1.0 - beta_one) * grad
        new_second = beta_two * second_ref[at] + (1.0 - beta_two) * grad * grad
        new_first_ref[at] = new_first
        new_second_ref[at] = new_second
        update_ref[at] = new_first / correct_one / (jnp.sqrt(new_second / correct_two) + epsilon)


def adam(scale, first_old, second_old, pieces):
    return kernel_call(
        functools.partial(adam_kernel, scale),
        [VMEM] * 10,
        [struct((256, 256), F32)] * 3 + [struct((64, 128), F32)],
        5,
        (1 << 20, 2 << 20),
        [first_old, second_old, *pieces],
    )


def shards(proj_in, kv_grad, normed, norm_grad, first_moment, second_moment):
    return update_of(proj_in[0], kv_grad[0], normed, norm_grad, first_moment[0], second_moment[0])


def update_of(inputs, rows, normed, norm_grad, first_moment, second_moment):
    replicas = lax.axis_size(DP)
    gain = jnp.sum(norm_grad.astype(F32) * normed.astype(F32), axis=1).reshape(64, 128)
    starts = [ordered(0, rows, [gain]), ordered(1, rows, [])]

    def gathered(k):
        own = {0: starts[k]}
        up = down = starts[k]
        for step in (1, 2, 3, 4):
            if step < 4 or k == 0:
                up = shift(up, 1)
                own[4 if step == 4 else -step] = up
            if step < 4 or k == 1:
                down = shift(down, -1)
                own[step] = down
        blocks = []
        for step in STEPS:
            blocks += [own[step], swap(own[step], "c", 1)]
        return blocks

    gathers = [gathered(k) for k in range(2)]
    mine = turned(inputs, 0)
    other = swap(turned(inputs, 1), "yh", 1)

    in_x, in_y = [], []
    for k in range(2):
        outs = product(k, mine, other, gathers[k])
        by_x, by_y = outs[:4], outs[4:]
        in_x += [by_x[0]] + [swap(by_x[j], "x", j) for j in (1, 2, 3)]
        in_y += [by_y[0]] + [along_y(by_y[ab], ab) for ab in (1, 2, 3)]
    by_y = cut_sum(sum_rows_kernel, in_x, BY_X + 32)
    by_x = cut_sum(sum_columns_kernel, in_y, BY_Y)
    pieces = [by_y[0]] + [along_y(by_y[ab], ab) for ab in (1, 2, 3)]
    pieces += [by_x[0]] + [swap(by_x[j], "x", j) for j in (1, 2, 3)]
    new_first, new_second, update, gain = adam(1.0 / replicas, first_moment, second_moment, pieces)
    return (new_first[None], new_second[None], update[None], gain.reshape(1, 8192))


def solution(mesh):
    finer = Mesh(mesh.devices.reshape(4, 2, 2, 8, 2), AXES)
    return jax.shard_map(
        shards,
        mesh=finer,
        in_specs=(
            P(None, DP, TP),
            P(None, DP_TP, None),
            P(None, DP_TP, None),
            P(None, DP_TP, None),
            P(None, TP, DP),
            P(None, TP, DP),
        ),
        out_specs=(P(None, TP, DP), P(None, TP, DP), P(None, TP, DP), P()),
        check_vma=False,
    )
```
